32 devices in a mesh: groups: 2 (over y), expert: 8 (over z, x), tensor: 2 (over core).
Axes of the slice: x: 2, y: 2, z: 4, core: 2. Of those that a mesh axis runs over, the one named last changes fastest.
Arguments:
- tokens: bfloat16 [4096, 1440], P(('groups', 'expert')), parts along dimension 0, may hold values from -6 to 6
- routes: int32 [4096, 4], P(('groups', 'expert')), parts along dimension 0, may hold values from 0 to 7, all different within a row; in each aligned block of 256 rows (0 to 255, 256 to 511, ...) at most 192 rows name the same one
- gates: float32 [4096, 4], P(('groups', 'expert')), parts along dimension 0, may hold values from 0.1 to 1
- w_gate: bfloat16 [8, 1440, 1440], P('expert', None, 'tensor'), may hold values from -0.15625 to 0.15625
- w_up: bfloat16 [8, 1440, 1440], P('expert', None, 'tensor'), may hold values from -0.15625 to 0.15625
- w_down: bfloat16 [8, 1440, 1440], P('expert', 'tensor'), may hold values from -0.15625 to 0.15625
- shared_gate: bfloat16 [1440, 1440], P(None, 'tensor'), may hold values from -0.15625 to 0.15625
- shared_up: bfloat16 [1440, 1440], P(None, 'tensor'), may hold values from -0.15625 to 0.15625
- shared_down: bfloat16 [1440, 1440], P('tensor'), may hold values from -0.15625 to 0.15625
Outputs:
- mixed: bfloat16 [4096, 1440], P(('groups', 'expert'), 'tensor'), parts along dimension 0
The draws below stay inside these ranges and needn't reach their ends.
There are 2 independent parts, one for each index of `groups`. The reference program is written for one: setup_inputs(seed, part) draws one part's arguments, and reference() takes and returns one part's arrays. A program takes and returns all parts, laid end to end along the dimension named above; an argument that names none is the same for every part. Nothing has to cross between parts.
Inputs may be any that keep to these rules, and one draw needn't show every extreme that they name: `routes`: each token names 4 different experts. Among the 256 tokens of one index of expert (aligned blocks of rows), no expert is named by more than 192 tokens; in some blocks one expert is named by exactly 192.
All inputs are finite; a program needn't handle non-finite values.
Results may differ from the reference program's by a relative error of at most 0.0051.
Values may be sent and summed in bfloat16 or wider, within the bound.
A program may use at most 192 MiB of HBM per device.

```python
import math
import jax
import jax.numpy as jnp
import numpy as np
from jax import lax

D = 1440
FF = 1440
FS = 1440
TOP = 4
TOK_DEV = 256
EXPERTS = 8
TOKENS = 2048
CAP = 192
N_EXPERT = 8


def levels(stream_key, dims, cuts, least, high):
    level, own = 1.0, jax.random.fold_in(stream_key, 6)
    for dim, blocks in cuts:
        heights = jnp.exp(jax.random.uniform(jax.random.fold_in(own, dim), (blocks,), jnp.float32, least / len(cuts), high / len(cuts)))
        level = level * jnp.repeat(heights, dims[dim] // blocks).reshape([-1 if axis == dim else 1 for axis in range(len(dims))])
    return level


def deal_out(stream_key, own, number, rows, count, top, bound, slope):
    ranking = jax.random.permutation(stream_key, count)
    crowded, usual = shares(count, rows * top, bound, slope, True), shares(count, rows * top, bound, slope, False)
    places = jnp.arange(count)

    def named(tallies, turn):
        used = int((tallies > 0).sum())
        fixed = max(1, used // 4)
        shifted = fixed + (places - fixed + turn * (used - fixed)) % max(1, count - fixed)
        return jnp.zeros((count,), jnp.int32).at[ranking[jnp.where(places < fixed, places, shifted)]].set(jnp.asarray(tallies, jnp.int32))

    tallies = jnp.where(number % 4 == 0, named(crowded, number // 4), named(usual, number - number // 4 - 1))
    mixed = jax.random.permutation(jax.random.fold_in(own, 3), count)
    source_of, receiver = mixed[0:count // 2 * 2:2], mixed[1:count // 2 * 2:2]
    margin = jnp.minimum(tallies[source_of] - 1, bound - tallies[receiver]) // 2
    margin = jnp.where((source_of == ranking[0]) | (receiver == ranking[0]) | (tallies[receiver] == 0), 0, jnp.maximum(margin, 0))
    shifted = jax.random.randint(jax.random.fold_in(own, 4), (count // 2,), 0, 1 << 20) % (margin + 1)
    tallies = tallies.at[source_of].add(-shifted).at[receiver].add(shifted)
    labels = jnp.searchsorted(jnp.cumsum(tallies), jnp.arange(rows * top), side="right").astype(jnp.int32)
    table = labels.reshape(top, rows).T
    table = table[jax.random.permutation(jax.random.fold_in(own, 1), rows)]
    turn = jax.random.randint(jax.random.fold_in(own, 2), (rows, 1), 0, top)
    return jnp.take_along_axis(table, (jnp.arange(top)[None, :] + turn) % top, axis=1)


def shares(amount, total, most, lean, full):
    loads = [(1 << 20) // math.isqrt(rank ** lean) + 1 for rank in range(1, amount + 1)]
    largest = most if full else min(most, max(-(-total // amount), total * loads[0] // sum(loads)))
    least = 1 if total - largest >= amount - 1 else 0
    holding, spare = [largest] + [least] * (amount - 1), total - largest - least * (amount - 1)
    while spare > 0:
        movable = [i for i in range(1, amount) if holding[i] < largest] or [i for i in range(1, amount) if holding[i] < most]
        whole, budget = sum([loads[i] for i in movable]), spare
        for i in movable:
            more = min(most - holding[i], max(1, budget * loads[i] // whole), spare)
            holding[i] = holding[i] + more
            spare = spare - more
    return np.array(holding)


def scatter_about(stream_key, shape, scale, most, cuts=(), kind=jnp.bfloat16):
    drawn = scale * jax.random.normal(stream_key, shape, jnp.float32)
    if cuts:
        drawn = drawn * levels(stream_key, shape, cuts, -0.22, 0.18)
    return jnp.clip(drawn, -most, most).astype(kind)


def setup_inputs(seed: int = 0, part: int = 0) -> dict:
    key_of = jax.random.split(jax.random.key(seed), 10)
    part_keys = jax.random.split(jax.random.fold_in(key_of[9], part), 10)
    tokens = scatter_about(part_keys[0], (TOKENS, D), 1.0, 6.0, ((0, 8),))
    routes_keys = jax.random.split(jax.random.fold_in(part_keys[1], 1), TOKENS // TOK_DEV)
    routes_turns = jax.random.permutation(jax.random.fold_in(part_keys[1], 3), TOKENS // TOK_DEV)
    routes = jax.vmap(lambda own, number: deal_out(jax.random.fold_in(part_keys[1], 2), own, number, TOK_DEV, EXPERTS, TOP, CAP, 2))(routes_keys, routes_turns).reshape((TOKENS, TOP))
    gates = jnp.clip(0.1 + 0.9 * jax.random.uniform(part_keys[2], (TOKENS, TOP), jnp.float32) ** levels(part_keys[2], (TOKENS, TOP), ((0, 8),), -0.2, 0.2), 0.1, 1.0)
    w_gate = scatter_about(key_of[3], (EXPERTS, D, FF), D ** -0.5, 0.15625, ((0, 8), (2, 2)))
    w_up = scatter_about(key_of[4], (EXPERTS, D, FF), D ** -0.5, 0.15625, ((0, 8), (2, 2)))
    w_down = scatter_about(key_of[5], (EXPERTS, FF, D), FF ** -0.5, 0.15625, ((0, 8), (1, 2)))
    shared_gate = scatter_about(key_of[6], (D, FS), D ** -0.5, 0.15625, ((1, 2),))
    shared_up = scatter_about(key_of[7], (D, FS), D ** -0.5, 0.15625, ((1, 2),))
    shared_down = scatter_about(key_of[8], (FS, D), FS ** -0.5, 0.15625, ((0, 2),))
    return {"tokens": tokens, "routes": routes, "gates": gates, "w_gate": w_gate, "w_up": w_up, "w_down": w_down, "shared_gate": shared_gate, "shared_up": shared_up, "shared_down": shared_down}


def reference(tokens, routes, gates, w_gate, w_up, w_down, shared_gate, shared_up, shared_down):
    blocked = routes.reshape(N_EXPERT, TOK_DEV * TOP)
    onehot = (blocked[:, :, None] == jnp.arange(EXPERTS, dtype=jnp.int32)[None, None, :]).astype(jnp.int32)
    order_in = jnp.sum(jnp.cumsum(onehot, axis=1) * onehot, axis=2) - 1
    source = jnp.arange(N_EXPERT, dtype=jnp.int32)[:, None]
    width_all = N_EXPERT * CAP
    slot_index = (blocked * width_all + source * CAP + order_in).reshape(-1).astype(jnp.int32)
    owner = jnp.repeat(jnp.arange(TOKENS, dtype=jnp.int32), TOP)
    token_of = jnp.full((EXPERTS * width_all,), TOKENS, jnp.int32).at[slot_index].set(owner)
    token_of = token_of.reshape(EXPERTS, width_all)
    padded = jnp.concatenate([tokens, jnp.zeros((1, D), tokens.dtype)], 0)

    def expert_rows(operands):
        index_rows, gate_mat, up_mat, down_mat = operands
        gathered = padded[index_rows]
        gate_val = jnp.dot(gathered, gate_mat, preferred_element_type=jnp.float32)
        up_val = jnp.dot(gathered, up_mat, preferred_element_type=jnp.float32)
        hidden = (jax.nn.silu(gate_val) * up_val).astype(jnp.bfloat16)
        return jnp.dot(hidden, down_mat, preferred_element_type=jnp.float32).astype(jnp.bfloat16)

    outputs = lax.map(expert_rows, (token_of, w_gate, w_up, w_down))
    picked = outputs.reshape(EXPERTS * width_all, D)[slot_index].reshape(TOKENS, TOP, D).astype(jnp.float32)
    routed = jnp.sum(gates[:, :, None] * picked, axis=1)
    shared_g = jnp.dot(tokens, shared_gate, preferred_element_type=jnp.float32)
    shared_u = jnp.dot(tokens, shared_up, preferred_element_type=jnp.float32)
    shared_hidden = (jax.nn.silu(shared_g) * shared_u).astype(jnp.bfloat16)
    shared_out = jnp.dot(shared_hidden, shared_down, preferred_element_type=jnp.float32)
    return (tokens.astype(jnp.float32) + routed + shared_out).astype(jnp.bfloat16)
```

```python
import functools

import jax
import jax.numpy as jnp
from jax import lax
from jax.experimental import pallas as pl
from jax.experimental.pallas import tpu as pltpu
from jax.sharding import PartitionSpec as P

MESH = pl.DeviceIdType.MESH
VMEM_BUDGET = 52 * 1024 * 1024


def exchange_local(tokens, routes, gates, w_gate, w_up, w_down, shared_gate, shared_up, shared_down):
    tok_count, top_count = routes.shape
    width_all = tokens.shape[1]
    local_experts = w_gate.shape[0]
    expert_count = lax.axis_size("expert")
    experts_all = expert_count * local_experts
    capacity = max(2, (3 * tok_count * top_count + 2 * experts_all - 1) // (2 * experts_all))
    flat_routes = routes.reshape(-1)
    onehot = (flat_routes[:, None] == jnp.arange(experts_all, dtype=jnp.int32)[None, :]).astype(
        jnp.int32
    )
    order_in = jnp.sum(jnp.cumsum(onehot, axis=0) * onehot, axis=1) - 1
    slot_index = flat_routes * capacity + order_in
    half_width = width_all // lax.axis_size("tensor")
    own_cols = lax.dynamic_slice_in_dim(
        tokens, lax.axis_index("tensor") * half_width, half_width, 1
    )
    outgoing = jnp.zeros((experts_all * capacity, half_width), jnp.bfloat16)
    outgoing = outgoing.at[slot_index].set(jnp.repeat(own_cols, top_count, axis=0))
    outgoing = outgoing.reshape(experts_all, capacity, half_width)
    received = lax.all_to_all(outgoing, "expert", split_axis=0, concat_axis=0, tiled=True)
    received = lax.all_gather(received, "tensor", axis=2, tiled=True)
    item_rows = received.shape[1]
    stacked = received.reshape(expert_count, local_experts, item_rows, width_all)
    stacked = stacked.transpose(1, 0, 2, 3).reshape(
        local_experts, expert_count * item_rows, width_all
    )
    gate_val = jnp.einsum("emd,edf->emf", stacked, w_gate, preferred_element_type=jnp.float32)
    up_val = jnp.einsum("emd,edf->emf", stacked, w_up, preferred_element_type=jnp.float32)
    hidden = (jax.nn.silu(gate_val) * up_val).astype(jnp.bfloat16)
    partial_value = jnp.einsum("emf,efd->emd", hidden, w_down, preferred_element_type=jnp.float32)
    partial_value = partial_value.reshape(local_experts, expert_count, item_rows, width_all)
    partial_value = partial_value.transpose(1, 0, 2, 3).reshape(experts_all, item_rows, width_all)
    summed = lax.psum_scatter(partial_value, "tensor", scatter_dimension=2, tiled=True).astype(
        jnp.bfloat16
    )
    returned = lax.all_to_all(summed, "expert", split_axis=0, concat_axis=0, tiled=True)
    shared_g = jnp.dot(tokens, shared_gate, preferred_element_type=jnp.float32)
    shared_u = jnp.dot(tokens, shared_up, preferred_element_type=jnp.float32)
    shared_hidden = (jax.nn.silu(shared_g) * shared_u).astype(jnp.bfloat16)
    shared_part = jnp.dot(shared_hidden, shared_down, preferred_element_type=jnp.float32)
    picked = returned.reshape(experts_all * capacity, half_width)[slot_index]
    picked = picked.astype(jnp.float32).reshape(tok_count, top_count, half_width)
    routed = jnp.sum(gates[:, :, None] * picked, axis=1)
    total = routed + lax.psum_scatter(shared_part, "tensor", scatter_dimension=1, tiled=True)
    return (own_cols.astype(jnp.float32) + total).astype(jnp.bfloat16)


def silu_mul(g, u):
    return (g / (1.0 + jnp.exp(-g)) * u).astype(jnp.bfloat16)


def moe_kernel(nz, nx, cap, tok_ref, routes_ref, gates_ref, wg_ref, wu_ref, wd_ref, sg_ref, su_ref, sd_ref, out_ref,
               TOK, X, XC, XO, XIN, YS, YC, CSs, CSr, OWN, O, SHB, SHr, MT, POS, WT, PCOL, U, Wg, Wu, Wd, Sg, Su, Sd,
               t_loc, w_loc, s_loc, w_send, w_recv, m_send, m_recv, z_send, z_recv, x_send, x_recv, d_send, d_recv,
               y_send, y_recv, e_send, e_recv, c_send, c_recv, h_send, h_recv):
    bf, f32 = jnp.bfloat16, jnp.float32
    me = lax.axis_index("expert")
    core = lax.axis_index("tensor")
    z = me // nx
    x = me % nx
    ox = nx - 1 - x
    other = z * nx + ox
    n = nz * nx
    rows = X.shape[1]
    half = out_ref.shape[1]
    ch = cap // 2
    top = routes_ref.shape[0]
    chunks = z_recv.shape[1]
    part = rows // chunks

    barrier = pltpu.get_barrier_semaphore()
    for d in range(1, n):
        pl.semaphore_signal(barrier, inc=1, device_id={"expert": (me + d) % n}, device_id_type=MESH)
    pl.semaphore_signal(barrier, inc=1, device_id={"tensor": 1 - core}, device_id_type=MESH)
    pl.semaphore_signal(barrier, inc=1, device_id={"expert": other, "tensor": 1 - core}, device_id_type=MESH)

    tok_in = pltpu.make_async_copy(tok_ref, TOK, t_loc)
    tok_in.start()
    loc_s = [pltpu.make_async_copy(a, b, s_loc.at[i]) for i, (a, b) in enumerate(
        ((sg_ref, Sg), (su_ref, Su), (sd_ref, Sd)))]
    loc_w = [pltpu.make_async_copy(a.at[0], b.at[0], w_loc.at[i]) for i, (a, b) in enumerate(
        ((wg_ref, Wg), (wu_ref, Wu), (wd_ref, Wd)))]
    for cp in loc_s + loc_w:
        cp.start()

    def remote(src, dst, ssem, rsem, **dev):
        return pltpu.make_async_remote_copy(src_ref=src, dst_ref=dst, send_sem=ssem, recv_sem=rsem,
                                            device_id=dev, device_id_type=MESH)

    MT[me, :top] = routes_ref[...].astype(f32)
    MT[me, top:] = gates_ref[...]
    U[...] = jnp.where(lax.broadcasted_iota(jnp.int32, U.shape, 0) < lax.broadcasted_iota(jnp.int32, U.shape, 1),
                       1.0, 0.0).astype(bf)

    def ranks(named, gate):
        mine, theirs = named == me.astype(f32), named == other.astype(f32)
        on = jnp.concatenate([jnp.sum(jnp.where(mine, 1.0, 0.0), axis=1),
                              jnp.sum(jnp.where(theirs, 1.0, 0.0), axis=1)], axis=0)
        place = jnp.dot(on.astype(bf), U[...], preferred_element_type=f32)
        return jnp.where(on > 0, place, -1.0), jnp.sum(jnp.where(mine, gate, 0.0), axis=1)

    place, _ = ranks(routes_ref[...].astype(f32)[None], gates_ref[...][None])
    POS[pl.ds(me, 1), :] = place[:1]
    POS[pl.ds(n + me, 1), :] = place[1:]
    tok_in.wait()
    for cc in range(2):
        @pl.when(core == cc)
        def _():
            X[z] = TOK[:, cc * half:(cc + 1) * half]
    pl.semaphore_wait(barrier, n + 1)

    def m_copy(e, d):
        return remote(MT.at[e], MT.at[e], m_send.at[d], m_recv.at[e], expert=(me + d) % n)

    def z_copy(zo, side, k):
        r = pl.ds(k * part, part)
        return remote(X.at[zo, r], X.at[zo, r], z_send.at[side, zo, k], z_recv.at[zo, k],
                      expert=me + nx if side == 0 else me - nx)

    def x_copy(zo, k, source):
        return remote(XC.at[zo, pl.ds(k * ch, ch)], XIN.at[zo, source, pl.ds(ch, ch)], x_send.at[k, zo],
                      x_recv.at[source, zo], expert=other, tensor=k)

    def d_copy(zo, source):
        return remote(XO.at[zo], XIN.at[zo, source, pl.ds(0, ch)], d_send.at[zo], d_recv.at[zo], tensor=1 - core)

    def y_copy(zo, k, source):
        r = pl.ds(pl.multiple_of(cap + source * ch, ch), ch)
        return remote(YS.at[zo, k, pl.ds(ch, ch)], YC.at[zo, r], y_send.at[k, zo], y_recv.at[source, zo],
                      expert=other, tensor=k)

    def e_copy(zo, source):
        r = pl.ds(pl.multiple_of(source * ch, ch), ch)
        return remote(YS.at[zo, 1 - core, pl.ds(0, ch)], YC.at[zo, r], e_send.at[zo], e_recv.at[zo], tensor=1 - core)

    def c_copy(zo, slot):
        return remote(CSs.at[zo], CSr.at[slot], c_send.at[zo], c_recv.at[slot], expert=zo * nx + x)

    def forward_z(zo, k):
        @pl.when(jnp.logical_and(zo <= z, z + 1 < nz))
        def _():
            z_copy(zo, 0, k).start()

        @pl.when(jnp.logical_and(zo >= z, z >= 1))
        def _():
            z_copy(zo, 1, k).start()

    def take_z(zo):
        for k in range(chunks):
            z_copy(zo, 0, k).wait_recv()
            forward_z(zo, k)

    def spread(zo):
        e = zo * nx + x
        r = lax.broadcasted_iota(jnp.int32, (cap, rows), 0)
        near = jnp.where(r < ch, r + core * ch, r - ch + (1 - core) * ch).astype(f32)
        pick = jnp.concatenate([jnp.where(r.astype(f32) == POS[pl.ds(n + e, 1), :], 1.0, 0.0),
                                jnp.where(near == POS[pl.ds(e, 1), :], 1.0, 0.0)], axis=0).astype(bf)
        got = jnp.dot(pick, X[zo], preferred_element_type=f32).astype(bf)
        XC[zo] = got[:cap]
        for k in range(2):
            x_copy(zo, k, core).start()
        XIN[zo, core, :ch] = got[cap:cap + ch]
        XO[zo] = got[cap + ch:]
        d_copy(zo, core).start()

    for d in range(1, n):
        m_copy(me, d).start()
    for k in range(chunks):
        forward_z(z, k)
    spread(z)
    rem_w = [remote(a.at[0], b.at[1], w_send.at[i], w_recv.at[i], tensor=1 - core) for i, (a, b) in enumerate(
        ((wg_ref, Wg), (wu_ref, Wu), (wd_ref, Wd)))]
    for cp in rem_w:
        cp.start()

    table = [sorted(range(nz), key=lambda q: (abs(q - k), abs(2 * q + 1 - nz))) for k in range(nz)]

    def nth(i):
        r = table[0][i]
        for k in range(1, nz):
            r = jnp.where(z == k, table[k][i], r)
        return r

    for cp in loc_s:
        cp.wait()
    tok = TOK[...]
    sh = silu_mul(jnp.dot(tok, Sg[...], preferred_element_type=f32),
                  jnp.dot(tok, Su[...], preferred_element_type=f32))
    sh_all = jnp.dot(sh, Sd[...], preferred_element_type=f32)
    SHB[0] = sh_all[:, :half]
    SHB[1] = sh_all[:, half:]
    h_copy = remote(SHB.at[1 - core], SHr, h_send, h_recv, tensor=1 - core)
    h_copy.start()

    for d in range(1, n):
        m_copy((me + d) % n, d).wait_recv()
    place, weight = ranks(MT[:, :top], MT[:, top:])
    POS[...] = place
    WT[...] = weight
    PCOL[...] = place.T

    for cp in loc_w:
        cp.wait()
    for cp in rem_w:
        cp.wait_recv()

    def compute(zo):
        d_copy(zo, 1 - core).wait_recv()
        for s in range(2):
            x_copy(zo, s, s).wait_recv()
        for hh in range(2):
            parts = []
            for w in (Wg, Wu):
                parts.append(jnp.dot(XIN[zo, 0], w[hh, :half], preferred_element_type=f32)
                             + jnp.dot(XIN[zo, 1], w[hh, half:], preferred_element_type=f32))
            down = jnp.dot(silu_mul(*parts), Wd[hh], preferred_element_type=f32)
            if hh == 0:
                O[...] = down
            else:
                O[...] += down
        r = (lax.broadcasted_iota(jnp.int32, (ch, rows), 0) + core * ch).astype(f32)
        weight = jnp.concatenate(
            [jnp.sum(jnp.where(r == POS[pl.ds(e, 1), :], WT[pl.ds(e, 1), :], 0.0), axis=1, keepdims=True)
             for e in (zo * nx + x, zo * nx + ox)], axis=0)
        y = (weight * O[...].astype(bf).astype(f32)).astype(bf)
        YS[zo, 0] = y[:, :half]
        YS[zo, 1] = y[:, half:]

    def give_near(zo):
        e_copy(zo, core).start()
        YC[zo, pl.ds(pl.multiple_of(core * ch, ch), ch)] = YS[zo, core, :ch]

    def give_far(zo):
        for k in range(2):
            y_copy(zo, k, core).start()

    def column(zo):
        e_copy(zo, 1 - core).wait_recv()
        for s in range(2):
            y_copy(zo, s, s).wait_recv()
        e = zo * nx + x
        lane = lax.broadcasted_iota(jnp.int32, PCOL.shape, 1)
        mine = jnp.sum(jnp.where(lane == e, PCOL[...], 0.0), axis=1, keepdims=True)
        theirs = jnp.sum(jnp.where(lane == n + e, PCOL[...], 0.0), axis=1, keepdims=True)
        theirs = jnp.where(theirs < 0, -1.0, theirs + cap)
        slot = lax.broadcasted_iota(jnp.int32, (rows, 2 * cap), 1)
        put = jnp.where(slot.astype(f32) == jnp.where(slot < cap, mine, theirs), 1.0, 0.0).astype(bf)
        return jnp.dot(put, YC[zo], preferred_element_type=f32)

    def column_sum(zo):
        CSs[zo] = column(zo).astype(bf)
        c_copy(zo, z).start()

    edge = jnp.logical_or(z == 0, z == nz - 1)
    for i in range(nz):
        zi = nth(i)

        @pl.when(edge)
        def _():
            if i + 1 < nz:
                take_z(nth(i + 1))
                spread(nth(i + 1))

        @pl.when(jnp.logical_not(edge))
        def _():
            if i == 0:
                for j in range(1, min(3, nz)):
                    take_z(nth(j))
                    spread(nth(j))
            elif i + 2 < nz:
                take_z(nth(i + 2))
                spread(nth(i + 2))
        if i >= 3:
            column_sum(nth(i - 2))
        compute(zi)
        give_near(zi)
        if i > 0:
            give_far(zi)
    give_far(z)
    for i in range(max(1, nz - 2), nz):
        column_sum(nth(i))
    OWN[...] = column(z)
    h_copy.wait_recv()
    total = X[z].astype(f32) + OWN[...] + (SHB[core] + SHr[...])
    for i in range(1, nz):
        zi = nth(i)
        c_copy(zi, zi).wait_recv()
        total = total + CSr[zi].astype(f32)
    out_ref[...] = total.astype(bf)

    for cp in rem_w:
        cp.wait_send()
    h_copy.wait_send()
    for d in range(1, n):
        m_copy(me, d).wait_send()
    for zo in range(nz):
        for k in range(chunks):
            @pl.when(jnp.logical_and(zo <= z, z + 1 < nz))
            def _():
                z_copy(zo, 0, k).wait_send()

            @pl.when(jnp.logical_and(zo >= z, z >= 1))
            def _():
                z_copy(zo, 1, k).wait_send()
        for k in range(2):
            x_copy(zo, k, core).wait_send()
            y_copy(zo, k, core).wait_send()
        d_copy(zo, core).wait_send()
        e_copy(zo, core).wait_send()

        @pl.when(zo != z)
        def _():
            c_copy(zo, z).wait_send()


def pad(n, m):
    return -(-n // m) * m


def most_named(tok_count, top_count, experts_all):
    return max(2, (3 * tok_count * top_count + 2 * experts_all - 1) // (2 * experts_all))


def gather_plan(tok_count, width, expert_count, local_experts, hidden, top_count):
    cap = most_named(tok_count, top_count, expert_count)
    if local_experts != 1 or expert_count % 2 or tok_count % 256 or width % 32 or cap % 32 or cap > tok_count:
        return None
    nz, half = expert_count // 2, pad(width // 2, 128)
    wide, hid = pad(width, 128), pad(hidden, 128)
    weights = 3 * (2 * width * hid + pad(hidden, 16) * wide) * 2
    moved = nz * half * 2 * (3 * tok_count + 2 * cap + 2 * cap + 2 * cap + 2 * cap)
    flat = tok_count * (wide * 2 + 4 * half * 4 + 2 * half) + cap * wide * 4 + 4 * tok_count * tok_count
    return weights + moved + flat


def gather_local(tokens, routes, gates, w_gate, w_up, w_down, shared_gate, shared_up, shared_down):
    tok_count, width = tokens.shape
    hidden = w_gate.shape[2]
    n = lax.axis_size("expert")
    top = routes.shape[1]
    nx, nz = 2, n // 2
    half = width // 2
    cap = most_named(tok_count, top, n)
    ch = cap // 2
    chunks = 2
    bf, f32 = jnp.bfloat16, jnp.float32
    vm, dma = pltpu.VMEM, pltpu.SemaphoreType.DMA
    scratch = [
        vm((tok_count, width), bf), vm((nz, tok_count, half), bf), vm((nz, cap, half), bf), vm((nz, ch, half), bf),
        vm((nz, 2, cap, half), bf), vm((nz, 2, cap, half), bf), vm((nz, 2 * cap, half), bf),
        vm((nz, tok_count, half), bf), vm((nz, tok_count, half), bf), vm((tok_count, half), f32),
        vm((cap, width), f32), vm((2, tok_count, half), f32), vm((tok_count, half), f32),
        vm((n, 2 * top, tok_count), f32), vm((2 * n, tok_count), f32), vm((n, tok_count), f32),
        vm((tok_count, 2 * n), f32), vm((tok_count, tok_count), bf),
        vm((2, width, hidden), bf), vm((2, width, hidden), bf), vm((2, hidden, width), bf),
        vm((width, hidden), bf), vm((width, hidden), bf), vm((hidden, width), bf),
        dma, dma((3,)), dma((3,)), dma((3,)), dma((3,)), dma((n,)), dma((n,)),
        dma((2, nz, chunks)), dma((nz, chunks)), dma((2, nz)), dma((2, nz)), dma((nz,)), dma((nz,)),
        dma((2, nz)), dma((2, nz)), dma((nz,)), dma((nz,)), dma((nz,)), dma((nz,)), dma, dma,
    ]
    in_vmem, in_hbm = pl.BlockSpec(memory_space=pltpu.VMEM), pl.BlockSpec(memory_space=pl.ANY)
    return pl.pallas_call(
        functools.partial(moe_kernel, nz, nx, cap),
        out_shape=jax.ShapeDtypeStruct((tok_count, half), bf),
        in_specs=[in_hbm] + [in_vmem] * 2 + [in_hbm] * 6,
        out_specs=in_vmem,
        scratch_shapes=scratch,
        compiler_params=pltpu.CompilerParams(collective_id=0, has_side_effects=True, vmem_limit_bytes=60 * 1024 * 1024),
    )(tokens, routes.T, gates.T, w_gate, w_up, w_down, shared_gate, shared_up, shared_down)


def local(tokens, routes, gates, w_gate, *rest):
    need = gather_plan(*tokens.shape, lax.axis_size("expert"), w_gate.shape[0], w_gate.shape[2], routes.shape[1])
    if need is not None and lax.axis_size("tensor") == 2 and need <= VMEM_BUDGET:
        return gather_local(tokens, routes, gates, w_gate, *rest)
    return exchange_local(tokens, routes, gates, w_gate, *rest)


def solution(mesh):
    in_specs = (
        P(("groups", "expert"), None),
        P(("groups", "expert"), None),
        P(("groups", "expert"), None),
        P("expert", None, "tensor"),
        P("expert", None, "tensor"),
        P("expert", "tensor", None),
        P(None, "tensor"),
        P(None, "tensor"),
        P("tensor", None),
    )
    out_specs = P(("groups", "expert"), "tensor")
    return jax.shard_map(local, mesh=mesh, in_specs=in_specs, out_specs=out_specs, check_vma=False)
```

```python
import functools

import jax
import jax.numpy as jnp
from jax import lax
from jax.experimental import pallas as pl
from jax.experimental.pallas import tpu as pltpu
from jax.sharding import PartitionSpec as P

MESH = pl.DeviceIdType.MESH
VMEM_BUDGET = 52 * 1024 * 1024


def exchange_local(tokens, routes, gates, w_gate, w_up, w_down, shared_gate, shared_up, shared_down):
    tok_count, top_count = routes.shape
    width_all = tokens.shape[1]
    local_experts = w_gate.shape[0]
    expert_count = lax.axis_size("expert")
    experts_all = expert_count * local_experts
    capacity = max(2, (3 * tok_count * top_count + 2 * experts_all - 1) // (2 * experts_all))
    flat_routes = routes.reshape(-1)
    onehot = (flat_routes[:, None] == jnp.arange(experts_all, dtype=jnp.int32)[None, :]).astype(
        jnp.int32
    )
    order_in = jnp.sum(jnp.cumsum(onehot, axis=0) * onehot, axis=1) - 1
    slot_index = flat_routes * capacity + order_in
    half_width = width_all // lax.axis_size("tensor")
    own_cols = lax.dynamic_slice_in_dim(
        tokens, lax.axis_index("tensor") * half_width, half_width, 1
    )
    outgoing = jnp.zeros((experts_all * capacity, half_width), jnp.bfloat16)
    outgoing = outgoing.at[slot_index].set(jnp.repeat(own_cols, top_count, axis=0))
    outgoing = outgoing.reshape(experts_all, capacity, half_width)
    received = lax.all_to_all(outgoing, "expert", split_axis=0, concat_axis=0, tiled=True)
    received = lax.all_gather(received, "tensor", axis=2, tiled=True)
    item_rows = received.shape[1]
    stacked = received.reshape(expert_count, local_experts, item_rows, width_all)
    stacked = stacked.transpose(1, 0, 2, 3).reshape(
        local_experts, expert_count * item_rows, width_all
    )
    gate_val = jnp.einsum("emd,edf->emf", stacked, w_gate, preferred_element_type=jnp.float32)
    up_val = jnp.einsum("emd,edf->emf", stacked, w_up, preferred_element_type=jnp.float32)
    hidden = (jax.nn.silu(gate_val) * up_val).astype(jnp.bfloat16)
    partial_value = jnp.einsum("emf,efd->emd", hidden, w_down, preferred_element_type=jnp.float32)
    partial_value = partial_value.reshape(local_experts, expert_count, item_rows, width_all)
    partial_value = partial_value.transpose(1, 0, 2, 3).reshape(experts_all, item_rows, width_all)
    summed = lax.psum_scatter(partial_value, "tensor", scatter_dimension=2, tiled=True).astype(
        jnp.bfloat16
    )
    returned = lax.all_to_all(summed, "expert", split_axis=0, concat_axis=0, tiled=True)
    shared_g = jnp.dot(tokens, shared_gate, preferred_element_type=jnp.float32)
    shared_u = jnp.dot(tokens, shared_up, preferred_element_type=jnp.float32)
    shared_hidden = (jax.nn.silu(shared_g) * shared_u).astype(jnp.bfloat16)
    shared_part = jnp.dot(shared_hidden, shared_down, preferred_element_type=jnp.float32)
    picked = returned.reshape(experts_all * capacity, half_width)[slot_index]
    picked = picked.astype(jnp.float32).reshape(tok_count, top_count, half_width)
    routed = jnp.sum(gates[:, :, None] * picked, axis=1)
    total = routed + lax.psum_scatter(shared_part, "tensor", scatter_dimension=1, tiled=True)
    return (own_cols.astype(jnp.float32) + total).astype(jnp.bfloat16)


def silu_mul(g, u):
    return (g / (1.0 + jnp.exp(-g)) * u).astype(jnp.bfloat16)


def moe_kernel(nz, nx, cap, tok_ref, routes_ref, gates_ref, wg_ref, wu_ref, wd_ref, sg_ref, su_ref, sd_ref, out_ref,
               TOK, X, XC, XO, XIN, YS, YC, CSs, CSr, OWN, O, SHB, SHr, MT, POS, WT, U, Wg, Wu, Wd, Sg, Su, Sd,
               t_loc, w_loc, s_loc, w_send, w_recv, m_send, m_recv, z_send, z_recv, x_send, x_recv, d_send, d_recv,
               y_send, y_recv, e_send, e_recv, c_send, c_recv, h_send, h_recv):
    bf, f32 = jnp.bfloat16, jnp.float32
    me = lax.axis_index("expert")
    core = lax.axis_index("tensor")
    z = me // nx
    x = me % nx
    ox = nx - 1 - x
    other = z * nx + ox
    n = nz * nx
    half, rows = out_ref.shape
    ch = cap // 2
    top = routes_ref.shape[0]
    chunks = z_recv.shape[1]
    part = half // chunks

    barrier = pltpu.get_barrier_semaphore()
    for d in range(1, n):
        pl.semaphore_signal(barrier, inc=1, device_id={"expert": (me + d) % n}, device_id_type=MESH)
    pl.semaphore_signal(barrier, inc=1, device_id={"tensor": 1 - core}, device_id_type=MESH)
    pl.semaphore_signal(barrier, inc=1, device_id={"expert": other, "tensor": 1 - core}, device_id_type=MESH)

    own_in = pltpu.make_async_copy(tok_ref.at[pl.ds(pl.multiple_of(core * half, 16), half)], X.at[z], t_loc.at[0])
    tok_in = pltpu.make_async_copy(tok_ref, TOK, t_loc.at[1])
    own_in.start()
    tok_in.start()
    loc_s = [pltpu.make_async_copy(a, b, s_loc.at[i]) for i, (a, b) in enumerate(
        ((sg_ref, Sg), (su_ref, Su), (sd_ref, Sd)))]
    loc_w = [pltpu.make_async_copy(a.at[0], b.at[0], w_loc.at[i]) for i, (a, b) in enumerate(
        ((wg_ref, Wg), (wu_ref, Wu), (wd_ref, Wd)))]
    for cp in loc_s + loc_w:
        cp.start()

    def remote(src, dst, ssem, rsem, **dev):
        return pltpu.make_async_remote_copy(src_ref=src, dst_ref=dst, send_sem=ssem, recv_sem=rsem,
                                            device_id=dev, device_id_type=MESH)

    MT[me, :top] = routes_ref[...].astype(f32)
    MT[me, top:] = gates_ref[...]
    U[...] = jnp.where(lax.broadcasted_iota(jnp.int32, U.shape, 0) < lax.broadcasted_iota(jnp.int32, U.shape, 1),
                       1.0, 0.0).astype(bf)

    def ranks(named, gate):
        mine, theirs = named == me.astype(f32), named == other.astype(f32)
        on = jnp.concatenate([jnp.sum(jnp.where(mine, 1.0, 0.0), axis=1),
                              jnp.sum(jnp.where(theirs, 1.0, 0.0), axis=1)], axis=0)
        place = jnp.dot(on.astype(bf), U[...], preferred_element_type=f32)
        return jnp.where(on > 0, place, -1.0), jnp.sum(jnp.where(mine, gate, 0.0), axis=1)

    place, _ = ranks(routes_ref[...].astype(f32)[None], gates_ref[...][None])
    POS[pl.ds(me, 1), :] = place[:1]
    POS[pl.ds(n + me, 1), :] = place[1:]
    own_in.wait()
    pl.semaphore_wait(barrier, n + 1)

    def m_copy(e, d):
        return remote(MT.at[e], MT.at[e], m_send.at[d], m_recv.at[e], expert=(me + d) % n)

    def z_copy(zo, side, k):
        r = pl.ds(k * part, part)
        return remote(X.at[zo, r], X.at[zo, r], z_send.at[side, zo, k], z_recv.at[zo, k],
                      expert=me + nx if side == 0 else me - nx)

    def x_copy(zo, k, source):
        return remote(XC.at[zo, pl.ds(k * ch, ch)], XIN.at[zo, source, pl.ds(ch, ch)], x_send.at[k, zo],
                      x_recv.at[source, zo], expert=other, tensor=k)

    def d_copy(zo, source):
        return remote(XO.at[zo], XIN.at[zo, source, pl.ds(0, ch)], d_send.at[zo], d_recv.at[zo], tensor=1 - core)

    def y_copy(zo, k, source):
        r = pl.ds(pl.multiple_of(cap + source * ch, ch), ch)
        return remote(YS.at[zo, k, pl.ds(ch, ch)], YC.at[zo, r], y_send.at[k, zo], y_recv.at[source, zo],
                      expert=other, tensor=k)

    def e_copy(zo, source):
        r = pl.ds(pl.multiple_of(source * ch, ch), ch)
        return remote(YS.at[zo, 1 - core, pl.ds(0, ch)], YC.at[zo, r], e_send.at[zo], e_recv.at[zo], tensor=1 - core)

    def c_copy(zo, slot):
        return remote(CSs.at[zo], CSr.at[slot], c_send.at[zo], c_recv.at[slot], expert=zo * nx + x)

    def forward_z(zo, k):
        @pl.when(jnp.logical_and(zo <= z, z + 1 < nz))
        def _():
            z_copy(zo, 0, k).start()

        @pl.when(jnp.logical_and(zo >= z, z >= 1))
        def _():
            z_copy(zo, 1, k).start()

    def take_z(zo):
        for k in range(chunks):
            z_copy(zo, 0, k).wait_recv()
            forward_z(zo, k)

    def spread(zo):
        e = zo * nx + x
        r = lax.broadcasted_iota(jnp.int32, (cap, rows), 0)
        near = jnp.where(r < ch, r + core * ch, r - ch + (1 - core) * ch).astype(f32)
        pick = jnp.concatenate([jnp.where(r.astype(f32) == POS[pl.ds(n + e, 1), :], 1.0, 0.0),
                                jnp.where(near == POS[pl.ds(e, 1), :], 1.0, 0.0)], axis=0).astype(bf)
        got = lax.dot_general(pick, X[zo], (((1,), (1,)), ((), ())), preferred_element_type=f32).astype(bf)
        XC[zo] = got[:cap]
        for k in range(2):
            x_copy(zo, k, core).start()
        XIN[zo, core, :ch] = got[cap:cap + ch]
        XO[zo] = got[cap + ch:]
        d_copy(zo, core).start()

    for d in range(1, n):
        m_copy(me, d).start()
    for k in range(chunks):
        forward_z(z, k)
    spread(z)
    rem_w = [remote(a.at[0], b.at[1], w_send.at[i], w_recv.at[i], tensor=1 - core) for i, (a, b) in enumerate(
        ((wg_ref, Wg), (wu_ref, Wu), (wd_ref, Wd)))]
    for cp in rem_w:
        cp.start()

    table = [sorted(range(nz), key=lambda q: (abs(q - k), abs(2 * q + 1 - nz))) for k in range(nz)]

    def nth(i):
        r = table[0][i]
        for k in range(1, nz):
            r = jnp.where(z == k, table[k][i], r)
        return r

    for cp in loc_s:
        cp.wait()
    tok_in.wait()
    tok = TOK[...].T
    sh = silu_mul(jnp.dot(tok, Sg[...], preferred_element_type=f32),
                  jnp.dot(tok, Su[...], preferred_element_type=f32))
    sh_all = jnp.dot(sh, Sd[...], preferred_element_type=f32).T
    SHB[0] = sh_all[:half]
    SHB[1] = sh_all[half:]
    h_copy = remote(SHB.at[1 - core], SHr, h_send, h_recv, tensor=1 - core)
    h_copy.start()

    for d in range(1, n):
        m_copy((me + d) % n, d).wait_recv()
    place, weight = ranks(MT[:, :top], MT[:, top:])
    POS[...] = place
    WT[...] = weight

    for cp in loc_w:
        cp.wait()
    for cp in rem_w:
        cp.wait_recv()

    def compute(zo):
        d_copy(zo, 1 - core).wait_recv()
        for s in range(2):
            x_copy(zo, s, s).wait_recv()
        for hh in range(2):
            parts = []
            for w in (Wg, Wu):
                parts.append(jnp.dot(XIN[zo, 0], w[hh, :half], preferred_element_type=f32)
                             + jnp.dot(XIN[zo, 1], w[hh, half:], preferred_element_type=f32))
            down = jnp.dot(silu_mul(*parts), Wd[hh], preferred_element_type=f32)
            if hh == 0:
                O[...] = down
            else:
                O[...] += down
        r = (lax.broadcasted_iota(jnp.int32, (ch, rows), 0) + core * ch).astype(f32)
        weight = jnp.concatenate(
            [jnp.sum(jnp.where(r == POS[pl.ds(e, 1), :], WT[pl.ds(e, 1), :], 0.0), axis=1, keepdims=True)
             for e in (zo * nx + x, zo * nx + ox)], axis=0)
        y = (weight * O[...].astype(bf).astype(f32)).astype(bf)
        YS[zo, 0] = y[:, :half]
        YS[zo, 1] = y[:, half:]

    def give_near(zo):
        e_copy(zo, core).start()
        YC[zo, pl.ds(pl.multiple_of(core * ch, ch), ch)] = YS[zo, core, :ch]

    def give_far(zo):
        for k in range(2):
            y_copy(zo, k, core).start()

    def column(zo):
        e_copy(zo, 1 - core).wait_recv()
        for s in range(2):
            y_copy(zo, s, s).wait_recv()
        e = zo * nx + x
        slot = lax.broadcasted_iota(jnp.int32, (cap, rows), 0).astype(f32)
        put = jnp.concatenate([jnp.where(slot == POS[pl.ds(q, 1), :], 1.0, 0.0) for q in (e, n + e)], axis=0).astype(bf)
        return lax.dot_general(YC[zo], put, (((0,), (0,)), ((), ())), preferred_element_type=f32)

    def column_sum(zo):
        CSs[zo] = column(zo).astype(bf)
        c_copy(zo, z).start()

    edge = jnp.logical_or(z == 0, z == nz - 1)
    for i in range(nz):
        zi = nth(i)

        @pl.when(edge)
        def _():
            if i + 1 < nz:
                take_z(nth(i + 1))
                spread(nth(i + 1))

        @pl.when(jnp.logical_not(edge))
        def _():
            if i == 0:
                for j in range(1, min(3, nz)):
                    take_z(nth(j))
                    spread(nth(j))
            elif i + 2 < nz:
                take_z(nth(i + 2))
                spread(nth(i + 2))
        if i >= 3:
            column_sum(nth(i - 2))
        compute(zi)
        give_near(zi)
        if i > 0:
            give_far(zi)
    give_far(z)
    for i in range(max(1, nz - 2), nz):
        column_sum(nth(i))
    OWN[...] = column(z)
    h_copy.wait_recv()
    total = X[z].astype(f32) + OWN[...] + (SHB[core] + SHr[...])
    for i in range(1, nz):
        zi = nth(i)
        c_copy(zi, zi).wait_recv()
        total = total + CSr[zi].astype(f32)
    out_ref[...] = total.astype(bf)

    for cp in rem_w:
        cp.wait_send()
    h_copy.wait_send()
    for d in range(1, n):
        m_copy(me, d).wait_send()
    for zo in range(nz):
        for k in range(chunks):
            @pl.when(jnp.logical_and(zo <= z, z + 1 < nz))
            def _():
                z_copy(zo, 0, k).wait_send()

            @pl.when(jnp.logical_and(zo >= z, z >= 1))
            def _():
                z_copy(zo, 1, k).wait_send()
        for k in range(2):
            x_copy(zo, k, core).wait_send()
            y_copy(zo, k, core).wait_send()
        d_copy(zo, core).wait_send()
        e_copy(zo, core).wait_send()

        @pl.when(zo != z)
        def _():
            c_copy(zo, z).wait_send()


def pad(n, m):
    return -(-n // m) * m


def most_named(tok_count, top_count, experts_all):
    return max(2, (3 * tok_count * top_count + 2 * experts_all - 1) // (2 * experts_all))


def gather_plan(tok_count, width, expert_count, local_experts, hidden, top_count):
    cap = most_named(tok_count, top_count, expert_count)
    if local_experts != 1 or expert_count % 2 or tok_count % 256 or width % 32 or cap % 32 or cap > tok_count:
        return None
    nz, half = expert_count // 2, pad(width // 2, 128)
    wide, hid = pad(width, 128), pad(hidden, 128)
    weights = 3 * (2 * width * hid + pad(hidden, 16) * wide) * 2
    moved = nz * half * 2 * (3 * tok_count + 2 * cap + 2 * cap + 2 * cap + 2 * cap)
    flat = tok_count * (wide * 2 + 4 * half * 4 + 2 * half) + cap * wide * 4 + 4 * tok_count * tok_count
    return weights + moved + flat


def gather_local(tokens, routes, gates, w_gate, w_up, w_down, shared_gate, shared_up, shared_down):
    tok_count, width = tokens.shape
    hidden = w_gate.shape[2]
    n = lax.axis_size("expert")
    top = routes.shape[1]
    nx, nz = 2, n // 2
    half = width // 2
    cap = most_named(tok_count, top, n)
    ch = cap // 2
    chunks = next(c for c in (3, 2, 1) if half % (16 * c) == 0)
    bf, f32 = jnp.bfloat16, jnp.float32
    vm, dma = pltpu.VMEM, pltpu.SemaphoreType.DMA
    scratch = [
        vm((width, tok_count), bf), vm((nz, half, tok_count), bf), vm((nz, cap, half), bf), vm((nz, ch, half), bf),
        vm((nz, 2, cap, half), bf), vm((nz, 2, cap, half), bf), vm((nz, 2 * cap, half), bf),
        vm((nz, half, tok_count), bf), vm((nz, half, tok_count), bf), vm((half, tok_count), f32),
        vm((cap, width), f32), vm((2, half, tok_count), f32), vm((half, tok_count), f32),
        vm((n, 2 * top, tok_count), f32), vm((2 * n, tok_count), f32), vm((n, tok_count), f32),
        vm((tok_count, tok_count), bf),
        vm((2, width, hidden), bf), vm((2, width, hidden), bf), vm((2, hidden, width), bf),
        vm((width, hidden), bf), vm((width, hidden), bf), vm((hidden, width), bf),
        dma((2,)), dma((3,)), dma((3,)), dma((3,)), dma((3,)), dma((n,)), dma((n,)),
        dma((2, nz, chunks)), dma((nz, chunks)), dma((2, nz)), dma((2, nz)), dma((nz,)), dma((nz,)),
        dma((2, nz)), dma((2, nz)), dma((nz,)), dma((nz,)), dma((nz,)), dma((nz,)), dma, dma,
    ]
    in_vmem, in_hbm = pl.BlockSpec(memory_space=pltpu.VMEM), pl.BlockSpec(memory_space=pl.ANY)
    return pl.pallas_call(
        functools.partial(moe_kernel, nz, nx, cap),
        out_shape=jax.ShapeDtypeStruct((half, tok_count), bf),
        in_specs=[in_hbm] + [in_vmem] * 2 + [in_hbm] * 6,
        out_specs=in_vmem,
        scratch_shapes=scratch,
        compiler_params=pltpu.CompilerParams(collective_id=0, has_side_effects=True, vmem_limit_bytes=60 * 1024 * 1024),
    )(tokens.T, routes.T, gates.T, w_gate, w_up, w_down, shared_gate, shared_up, shared_down).T


def local(tokens, routes, gates, w_gate, *rest):
    need = gather_plan(*tokens.shape, lax.axis_size("expert"), w_gate.shape[0], w_gate.shape[2], routes.shape[1])
    if need is not None and lax.axis_size("tensor") == 2 and need <= VMEM_BUDGET:
        return gather_local(tokens, routes, gates, w_gate, *rest)
    return exchange_local(tokens, routes, gates, w_gate, *rest)


def solution(mesh):
    in_specs = (
        P(("groups", "expert"), None),
        P(("groups", "expert"), None),
        P(("groups", "expert"), None),
        P("expert", None, "tensor"),
        P("expert", None, "tensor"),
        P("expert", "tensor", None),
        P(None, "tensor"),
        P(None, "tensor"),
        P("tensor", None),
    )
    out_specs = P(("groups", "expert"), "tensor")
    return jax.shard_map(local, mesh=mesh, in_specs=in_specs, out_specs=out_specs, check_vma=False)
```

```python
import functools

import jax
import jax.numpy as jnp
from jax import lax
from jax.experimental import pallas as pl
from jax.experimental.pallas import tpu as pltpu
from jax.sharding import PartitionSpec as P

MESH = pl.DeviceIdType.MESH
VMEM_BUDGET = 52 * 1024 * 1024
LINE = 4
EDGE_ORDER = (
    ("take", 1), ("spread", 1), ("take", 2), ("spread", 2), ("compute", 0), ("take", 3), ("spread", 3),
    ("compute", 2), ("give", 2), ("compute", 3), ("compute", 1), ("give", 3), ("give", 1), ("sum", 2), ("sum",
    3), ("sum", 1), ("give", 0), ("sum", 0),
)
INNER_ORDER = (
    ("take", 1), ("spread", 1), ("take", 2), ("spread", 2), ("take", 3), ("spread", 3), ("compute", 0),
    ("compute", 1), ("compute", 2), ("give", 2), ("give", 1), ("sum", 2), ("compute", 3), ("give", 3),
    ("give", 0), ("sum", 1), ("sum", 3), ("sum", 0),
)
RELAYED, MERGED, SOURCES = (2, 3), (1, 3), (1, 2)


def exchange_local(tokens, routes, gates, w_gate, w_up, w_down, shared_gate, shared_up, shared_down):
    tok_count, top_count = routes.shape
    width_all = tokens.shape[1]
    local_experts = w_gate.shape[0]
    expert_count = lax.axis_size("expert")
    experts_all = expert_count * local_experts
    capacity = max(2, (3 * tok_count * top_count + 2 * experts_all - 1) // (2 * experts_all))
    flat_routes = routes.reshape(-1)
    onehot = (flat_routes[:, None] == jnp.arange(experts_all, dtype=jnp.int32)[None, :]).astype(
        jnp.int32
    )
    order_in = jnp.sum(jnp.cumsum(onehot, axis=0) * onehot, axis=1) - 1
    slot_index = flat_routes * capacity + order_in
    half_width = width_all // lax.axis_size("tensor")
    own_cols = lax.dynamic_slice_in_dim(
        tokens, lax.axis_index("tensor") * half_width, half_width, 1
    )
    outgoing = jnp.zeros((experts_all * capacity, half_width), jnp.bfloat16)
    outgoing = outgoing.at[slot_index].set(jnp.repeat(own_cols, top_count, axis=0))
    outgoing = outgoing.reshape(experts_all, capacity, half_width)
    received = lax.all_to_all(outgoing, "expert", split_axis=0, concat_axis=0, tiled=True)
    received = lax.all_gather(received, "tensor", axis=2, tiled=True)
    item_rows = received.shape[1]
    stacked = received.reshape(expert_count, local_experts, item_rows, width_all)
    stacked = stacked.transpose(1, 0, 2, 3).reshape(
        local_experts, expert_count * item_rows, width_all
    )
    gate_val = jnp.einsum("emd,edf->emf", stacked, w_gate, preferred_element_type=jnp.float32)
    up_val = jnp.einsum("emd,edf->emf", stacked, w_up, preferred_element_type=jnp.float32)
    hidden = (jax.nn.silu(gate_val) * up_val).astype(jnp.bfloat16)
    partial_value = jnp.einsum("emf,efd->emd", hidden, w_down, preferred_element_type=jnp.float32)
    partial_value = partial_value.reshape(local_experts, expert_count, item_rows, width_all)
    partial_value = partial_value.transpose(1, 0, 2, 3).reshape(experts_all, item_rows, width_all)
    summed = lax.psum_scatter(partial_value, "tensor", scatter_dimension=2, tiled=True).astype(
        jnp.bfloat16
    )
    returned = lax.all_to_all(summed, "expert", split_axis=0, concat_axis=0, tiled=True)
    shared_g = jnp.dot(tokens, shared_gate, preferred_element_type=jnp.float32)
    shared_u = jnp.dot(tokens, shared_up, preferred_element_type=jnp.float32)
    shared_hidden = (jax.nn.silu(shared_g) * shared_u).astype(jnp.bfloat16)
    shared_part = jnp.dot(shared_hidden, shared_down, preferred_element_type=jnp.float32)
    picked = returned.reshape(experts_all * capacity, half_width)[slot_index]
    picked = picked.astype(jnp.float32).reshape(tok_count, top_count, half_width)
    routed = jnp.sum(gates[:, :, None] * picked, axis=1)
    total = routed + lax.psum_scatter(shared_part, "tensor", scatter_dimension=1, tiled=True)
    return (own_cols.astype(jnp.float32) + total).astype(jnp.bfloat16)


def silu_mul(g, u):
    return (g / (1.0 + jnp.exp(-g)) * u).astype(jnp.bfloat16)


def moe_kernel(nz, nx, cap, tok_ref, routes_ref, gates_ref, wg_ref, wu_ref, wd_ref, sg_ref, su_ref, sd_ref, out_ref,
               TOK, X, XC, XO, XIN, YS, YC, CSs, CSr, MRG, OWN, O, SHB, SHr, MT, POS, WT, U, Wg, Wu, Wd, Sg, Su, Sd,
               t_loc, w_loc, s_loc, w_send, w_recv, m_send, m_recv, z_send, z_recv, x_send, x_recv, d_send, d_recv,
               y_send, y_recv, e_send, e_recv, c_send, c_recv, g_recv, h_send, h_recv):
    bf, f32 = jnp.bfloat16, jnp.float32
    me = lax.axis_index("expert")
    core = lax.axis_index("tensor")
    z = me // nx
    x = me % nx
    ox = nx - 1 - x
    other = z * nx + ox
    n = nz * nx
    half, rows = out_ref.shape
    ch = cap // 2
    top = routes_ref.shape[0]
    chunks = z_recv.shape[1]
    part = half // chunks
    sum_chunks = c_send.shape[1]
    sum_part = half // sum_chunks

    barrier = pltpu.get_barrier_semaphore()
    for d in range(1, n):
        pl.semaphore_signal(barrier, inc=1, device_id={"expert": (me + d) % n}, device_id_type=MESH)
    pl.semaphore_signal(barrier, inc=1, device_id={"tensor": 1 - core}, device_id_type=MESH)
    pl.semaphore_signal(barrier, inc=1, device_id={"expert": other, "tensor": 1 - core}, device_id_type=MESH)

    own_in = pltpu.make_async_copy(tok_ref.at[pl.ds(pl.multiple_of(core * half, 16), half)], X.at[z], t_loc.at[0])
    tok_in = pltpu.make_async_copy(tok_ref, TOK, t_loc.at[1])
    own_in.start()
    tok_in.start()
    loc_s = [pltpu.make_async_copy(a, b, s_loc.at[i]) for i, (a, b) in enumerate(
        ((sg_ref, Sg), (su_ref, Su), (sd_ref, Sd)))]
    loc_w = [pltpu.make_async_copy(a.at[0], b.at[0], w_loc.at[i]) for i, (a, b) in enumerate(
        ((wg_ref, Wg), (wu_ref, Wu), (wd_ref, Wd)))]
    for cp in loc_s + loc_w:
        cp.start()

    def remote(src, dst, ssem, rsem, **dev):
        return pltpu.make_async_remote_copy(src_ref=src, dst_ref=dst, send_sem=ssem, recv_sem=rsem,
                                            device_id=dev, device_id_type=MESH)

    MT[me, :top] = routes_ref[...].astype(f32)
    MT[me, top:] = gates_ref[...]
    U[...] = jnp.where(lax.broadcasted_iota(jnp.int32, U.shape, 0) < lax.broadcasted_iota(jnp.int32, U.shape, 1),
                       1.0, 0.0).astype(bf)

    def ranks(named, gate):
        mine, theirs = named == me.astype(f32), named == other.astype(f32)
        on = jnp.concatenate([jnp.sum(jnp.where(mine, 1.0, 0.0), axis=1),
                              jnp.sum(jnp.where(theirs, 1.0, 0.0), axis=1)], axis=0)
        place = jnp.dot(on.astype(bf), U[...], preferred_element_type=f32)
        return jnp.where(on > 0, place, -1.0), jnp.sum(jnp.where(mine, gate, 0.0), axis=1)

    place, _ = ranks(routes_ref[...].astype(f32)[None], gates_ref[...][None])
    POS[pl.ds(me, 1), :] = place[:1]
    POS[pl.ds(n + me, 1), :] = place[1:]
    own_in.wait()
    pl.semaphore_wait(barrier, n + 1)

    def m_copy(e, d):
        return remote(MT.at[e], MT.at[e], m_send.at[d], m_recv.at[e], expert=(me + d) % n)

    def z_copy(zo, side, k):
        r = pl.ds(k * part, part)
        return remote(X.at[zo, r], X.at[zo, r], z_send.at[side, zo, k], z_recv.at[zo, k],
                      expert=me + nx if side == 0 else me - nx)

    def x_copy(zo, k, source):
        return remote(XC.at[zo, pl.ds(k * ch, ch)], XIN.at[zo, source, pl.ds(ch, ch)], x_send.at[k, zo],
                      x_recv.at[source, zo], expert=other, tensor=k)

    def d_copy(zo, source):
        return remote(XO.at[zo], XIN.at[zo, source, pl.ds(0, ch)], d_send.at[zo], d_recv.at[zo], tensor=1 - core)

    def y_copy(zo, k, source):
        r = pl.ds(pl.multiple_of(cap + source * ch, ch), ch)
        return remote(YS.at[zo, k, pl.ds(ch, ch)], YC.at[zo, r], y_send.at[k, zo], y_recv.at[source, zo],
                      expert=other, tensor=k)

    def e_copy(zo, source):
        r = pl.ds(pl.multiple_of(source * ch, ch), ch)
        return remote(YS.at[zo, 1 - core, pl.ds(0, ch)], YC.at[zo, r], e_send.at[zo], e_recv.at[zo], tensor=1 - core)

    def c_copy(zo, slot, k):
        r = pl.ds(k * sum_part, sum_part)
        return remote(CSs.at[zo, r], CSr.at[slot, r], c_send.at[zo, k], c_recv.at[slot, k], expert=zo * nx + x)

    def g_copy(zo, k):
        r = pl.ds(k * sum_part, sum_part)
        return remote(CSs.at[zo, r], MRG.at[zo, r], c_send.at[zo, k], g_recv.at[zo, k],
                      expert=jnp.where(z == 0, me + nx, me - nx))

    def forward_z(zo, k):
        @pl.when(jnp.logical_and(zo <= z, z + 1 < nz))
        def _():
            z_copy(zo, 0, k).start()

        @pl.when(jnp.logical_and(zo >= z, z >= 1))
        def _():
            z_copy(zo, 1, k).start()

    def take_z(zo):
        for k in range(chunks):
            z_copy(zo, 0, k).wait_recv()
            forward_z(zo, k)

    def spread(zo):
        e = zo * nx + x
        r = lax.broadcasted_iota(jnp.int32, (cap, rows), 0)
        near = jnp.where(r < ch, r + core * ch, r - ch + (1 - core) * ch).astype(f32)
        pick = jnp.concatenate([jnp.where(r.astype(f32) == POS[pl.ds(n + e, 1), :], 1.0, 0.0),
                                jnp.where(near == POS[pl.ds(e, 1), :], 1.0, 0.0)], axis=0).astype(bf)
        got = lax.dot_general(pick, X[zo], (((1,), (1,)), ((), ())), preferred_element_type=f32).astype(bf)
        XC[zo] = got[:cap]
        for k in range(2):
            x_copy(zo, k, core).start()
        XIN[zo, core, :ch] = got[cap:cap + ch]
        XO[zo] = got[cap + ch:]
        d_copy(zo, core).start()

    for d in range(1, n):
        m_copy(me, d).start()
    for k in range(chunks):
        forward_z(z, k)
    spread(z)
    rem_w = [remote(a.at[0], b.at[1], w_send.at[i], w_recv.at[i], tensor=1 - core) for i, (a, b) in enumerate(
        ((wg_ref, Wg), (wu_ref, Wu), (wd_ref, Wd)))]
    for cp in rem_w:
        cp.start()

    table = [sorted(range(nz), key=lambda q: (abs(q - k), abs(2 * q + 1 - nz))) for k in range(nz)]

    def nth(i):
        r = table[0][i]
        for k in range(1, nz):
            r = jnp.where(z == k, table[k][i], r)
        return r

    for cp in loc_s:
        cp.wait()
    tok_in.wait()
    tok = TOK[...].T
    sh = silu_mul(jnp.dot(tok, Sg[...], preferred_element_type=f32),
                  jnp.dot(tok, Su[...], preferred_element_type=f32))
    sh_all = jnp.dot(sh, Sd[...], preferred_element_type=f32).T
    SHB[0] = sh_all[:half]
    SHB[1] = sh_all[half:]
    h_copy = remote(SHB.at[1 - core], SHr, h_send, h_recv, tensor=1 - core)
    h_copy.start()

    for d in range(1, n):
        m_copy((me + d) % n, d).wait_recv()
    place, weight = ranks(MT[:, :top], MT[:, top:])
    POS[...] = place
    WT[...] = weight

    for cp in loc_w:
        cp.wait()
    for cp in rem_w:
        cp.wait_recv()

    def compute(zo):
        d_copy(zo, 1 - core).wait_recv()
        for s in range(2):
            x_copy(zo, s, s).wait_recv()
        for hh in range(2):
            parts = []
            for w in (Wg, Wu):
                parts.append(jnp.dot(XIN[zo, 0], w[hh, :half], preferred_element_type=f32)
                             + jnp.dot(XIN[zo, 1], w[hh, half:], preferred_element_type=f32))
            down = jnp.dot(silu_mul(*parts), Wd[hh], preferred_element_type=f32)
            if hh == 0:
                O[...] = down
            else:
                O[...] += down
        r = (lax.broadcasted_iota(jnp.int32, (ch, rows), 0) + core * ch).astype(f32)
        weight = jnp.concatenate(
            [jnp.sum(jnp.where(r == POS[pl.ds(e, 1), :], WT[pl.ds(e, 1), :], 0.0), axis=1, keepdims=True)
             for e in (zo * nx + x, zo * nx + ox)], axis=0)
        y = (weight * O[...].astype(bf).astype(f32)).astype(bf)
        YS[zo, 0] = y[:, :half]
        YS[zo, 1] = y[:, half:]

    def give_near(zo):
        e_copy(zo, core).start()
        YC[zo, pl.ds(pl.multiple_of(core * ch, ch), ch)] = YS[zo, core, :ch]

    def give_far(zo):
        for k in range(2):
            y_copy(zo, k, core).start()

    def column(zo):
        e_copy(zo, 1 - core).wait_recv()
        for s in range(2):
            y_copy(zo, s, s).wait_recv()
        e = zo * nx + x
        slot = lax.broadcasted_iota(jnp.int32, (cap, rows), 0).astype(f32)
        put = jnp.concatenate([jnp.where(slot == POS[pl.ds(q, 1), :], 1.0, 0.0) for q in (e, n + e)], axis=0).astype(bf)
        return lax.dot_general(YC[zo], put, (((0,), (0,)), ((), ())), preferred_element_type=f32)

    def column_sum(i, on_edge):
        zo = nth(i)
        if i == 0:
            OWN[...] = X[z].astype(f32) + column(z)
            return
        summed = column(zo)
        for k in range(sum_chunks):
            r = slice(k * sum_part, (k + 1) * sum_part)
            piece = summed[r]
            if not on_edge and i in MERGED:
                g_copy(zo, k).wait_recv()
                piece = piece + MRG[zo, r].astype(f32)
            CSs[zo, r] = piece.astype(bf)
            if on_edge and i in RELAYED:
                g_copy(zo, k).start()
            else:
                c_copy(zo, z, k).start()

    edge = jnp.logical_or(z == 0, z == nz - 1)

    def run(steps, on_edge):
        for op, i in steps:
            if op == "take":
                take_z(nth(i))
            elif op == "spread":
                spread(nth(i))
            elif op == "give":
                give_far(nth(i))
            else:
                column_sum(i, on_edge)

    def cut(order):
        gaps, firsts = [[]], []
        for op, i in order:
            if op == "compute":
                firsts.append(i)
                gaps.append([])
            else:
                gaps[-1].append((op, i))
        return gaps, firsts

    edge_gaps, edge_first = cut(EDGE_ORDER)
    inner_gaps, inner_first = cut(INNER_ORDER)
    for j in range(nz + 1):
        @pl.when(edge)
        def _():
            run(edge_gaps[j], True)

        @pl.when(jnp.logical_not(edge))
        def _():
            run(inner_gaps[j], False)
        if j < nz:
            zi = jnp.where(edge, nth(edge_first[j]), nth(inner_first[j]))
            compute(zi)
            give_near(zi)
    h_copy.wait_recv()
    OWN[...] += SHB[core] + SHr[...]
    for k in range(sum_chunks):
        r = slice(k * sum_part, (k + 1) * sum_part)
        total = OWN[r]
        for i in SOURCES:
            zi = nth(i)
            c_copy(zi, zi, k).wait_recv()
            total = total + CSr[zi, r].astype(f32)
        out_ref[r] = total.astype(bf)

    for cp in rem_w:
        cp.wait_send()
    h_copy.wait_send()
    for d in range(1, n):
        m_copy(me, d).wait_send()
    for zo in range(nz):
        for k in range(chunks):
            @pl.when(jnp.logical_and(zo <= z, z + 1 < nz))
            def _():
                z_copy(zo, 0, k).wait_send()

            @pl.when(jnp.logical_and(zo >= z, z >= 1))
            def _():
                z_copy(zo, 1, k).wait_send()
        for k in range(2):
            x_copy(zo, k, core).wait_send()
            y_copy(zo, k, core).wait_send()
        d_copy(zo, core).wait_send()
        e_copy(zo, core).wait_send()

        @pl.when(zo != z)
        def _():
            for k in range(sum_chunks):
                c_copy(zo, z, k).wait_send()


def pad(n, m):
    return -(-n // m) * m


def most_named(tok_count, top_count, experts_all):
    return max(2, (3 * tok_count * top_count + 2 * experts_all - 1) // (2 * experts_all))


def gather_plan(tok_count, width, expert_count, local_experts, hidden, top_count):
    cap = most_named(tok_count, top_count, expert_count)
    if local_experts != 1 or expert_count != 2 * LINE or tok_count % 256 or width % 32 or cap % 32 or cap > tok_count:
        return None
    nz, half = expert_count // 2, pad(width // 2, 128)
    wide, hid = pad(width, 128), pad(hidden, 128)
    weights = 3 * (2 * width * hid + pad(hidden, 16) * wide) * 2
    moved = nz * half * 2 * (4 * tok_count + 2 * cap + 2 * cap + 2 * cap + 2 * cap)
    flat = tok_count * (wide * 2 + 4 * half * 4 + 2 * half) + cap * wide * 4 + 4 * tok_count * tok_count
    return weights + moved + flat


def gather_local(tokens, routes, gates, w_gate, w_up, w_down, shared_gate, shared_up, shared_down):
    tok_count, width = tokens.shape
    hidden = w_gate.shape[2]
    n = lax.axis_size("expert")
    top = routes.shape[1]
    nx, nz = 2, n // 2
    half = width // 2
    cap = most_named(tok_count, top, n)
    ch = cap // 2
    chunks = next(c for c in (3, 2, 1) if half % (16 * c) == 0)
    sums = chunks
    bf, f32 = jnp.bfloat16, jnp.float32
    vm, dma = pltpu.VMEM, pltpu.SemaphoreType.DMA
    scratch = [
        vm((width, tok_count), bf), vm((nz, half, tok_count), bf), vm((nz, cap, half), bf), vm((nz, ch, half), bf),
        vm((nz, 2, cap, half), bf), vm((nz, 2, cap, half), bf), vm((nz, 2 * cap, half), bf),
        vm((nz, half, tok_count), bf), vm((nz, half, tok_count), bf), vm((nz, half, tok_count), bf), vm((half, tok_count), f32),
        vm((cap, width), f32), vm((2, half, tok_count), f32), vm((half, tok_count), f32),
        vm((n, 2 * top, tok_count), f32), vm((2 * n, tok_count), f32), vm((n, tok_count), f32),
        vm((tok_count, tok_count), bf),
        vm((2, width, hidden), bf), vm((2, width, hidden), bf), vm((2, hidden, width), bf),
        vm((width, hidden), bf), vm((width, hidden), bf), vm((hidden, width), bf),
        dma((2,)), dma((3,)), dma((3,)), dma((3,)), dma((3,)), dma((n,)), dma((n,)),
        dma((2, nz, chunks)), dma((nz, chunks)), dma((2, nz)), dma((2, nz)), dma((nz,)), dma((nz,)),
        dma((2, nz)), dma((2, nz)), dma((nz,)), dma((nz,)), dma((nz, sums)), dma((nz, sums)), dma((nz, sums)), dma, dma,
    ]
    in_vmem, in_hbm = pl.BlockSpec(memory_space=pltpu.VMEM), pl.BlockSpec(memory_space=pl.ANY)
    return pl.pallas_call(
        functools.partial(moe_kernel, nz, nx, cap),
        out_shape=jax.ShapeDtypeStruct((half, tok_count), bf),
        in_specs=[in_hbm] + [in_vmem] * 2 + [in_hbm] * 6,
        out_specs=in_vmem,
        scratch_shapes=scratch,
        compiler_params=pltpu.CompilerParams(collective_id=0, has_side_effects=True, vmem_limit_bytes=60 * 1024 * 1024),
    )(tokens.T, routes.T, gates.T, w_gate, w_up, w_down, shared_gate, shared_up, shared_down).T


def local(tokens, routes, gates, w_gate, *rest):
    need = gather_plan(*tokens.shape, lax.axis_size("expert"), w_gate.shape[0], w_gate.shape[2], routes.shape[1])
    if need is not None and lax.axis_size("tensor") == 2 and need <= VMEM_BUDGET:
        return gather_local(tokens, routes, gates, w_gate, *rest)
    return exchange_local(tokens, routes, gates, w_gate, *rest)


def solution(mesh):
    in_specs = (
        P(("groups", "expert"), None),
        P(("groups", "expert"), None),
        P(("groups", "expert"), None),
        P("expert", None, "tensor"),
        P("expert", None, "tensor"),
        P("expert", "tensor", None),
        P(None, "tensor"),
        P(None, "tensor"),
        P("tensor", None),
    )
    out_specs = P(("groups", "expert"), "tensor")
    return jax.shard_map(local, mesh=mesh, in_specs=in_specs, out_specs=out_specs, check_vma=False)
```

```python
import functools

import jax
import jax.numpy as jnp
from jax import lax
from jax.experimental import pallas as pl
from jax.experimental.pallas import tpu as pltpu
from jax.sharding import PartitionSpec as P

MESH = pl.DeviceIdType.MESH
VMEM_BUDGET = 52 * 1024 * 1024
LINE = 4
EDGE_ORDER = (
    ("take", 1), ("spread", 1), ("compute", 0), ("take", 2), ("spread", 2), ("compute", 1), ("sum", 1),
    ("take", 3), ("spread", 3), ("compute", 2), ("give", 2), ("compute", 3), ("give", 3), ("sum", 2), ("give",
    0), ("sum", 3), ("sum", 0),
)
INNER_ORDER = (
    ("take", 1), ("spread", 1), ("take", 2), ("spread", 2), ("take", 3), ("spread", 3), ("compute", 1),
    ("compute", 2), ("give", 2), ("compute", 0), ("give", 1), ("compute", 3), ("give", 3), ("sum", 2),
    ("give", 0), ("sum", 1), ("sum", 3), ("sum", 0),
)
RELAYED, MERGED, SOURCES = (2, 3), (1, 3), (1, 2)


def exchange_local(tokens, routes, gates, w_gate, w_up, w_down, shared_gate, shared_up, shared_down):
    tok_count, top_count = routes.shape
    width_all = tokens.shape[1]
    local_experts = w_gate.shape[0]
    expert_count = lax.axis_size("expert")
    experts_all = expert_count * local_experts
    capacity = max(2, (3 * tok_count * top_count + 2 * experts_all - 1) // (2 * experts_all))
    flat_routes = routes.reshape(-1)
    onehot = (flat_routes[:, None] == jnp.arange(experts_all, dtype=jnp.int32)[None, :]).astype(
        jnp.int32
    )
    order_in = jnp.sum(jnp.cumsum(onehot, axis=0) * onehot, axis=1) - 1
    slot_index = flat_routes * capacity + order_in
    half_width = width_all // lax.axis_size("tensor")
    own_cols = lax.dynamic_slice_in_dim(
        tokens, lax.axis_index("tensor") * half_width, half_width, 1
    )
    outgoing = jnp.zeros((experts_all * capacity, half_width), jnp.bfloat16)
    outgoing = outgoing.at[slot_index].set(jnp.repeat(own_cols, top_count, axis=0))
    outgoing = outgoing.reshape(experts_all, capacity, half_width)
    received = lax.all_to_all(outgoing, "expert", split_axis=0, concat_axis=0, tiled=True)
    received = lax.all_gather(received, "tensor", axis=2, tiled=True)
    item_rows = received.shape[1]
    stacked = received.reshape(expert_count, local_experts, item_rows, width_all)
    stacked = stacked.transpose(1, 0, 2, 3).reshape(
        local_experts, expert_count * item_rows, width_all
    )
    gate_val = jnp.einsum("emd,edf->emf", stacked, w_gate, preferred_element_type=jnp.float32)
    up_val = jnp.einsum("emd,edf->emf", stacked, w_up, preferred_element_type=jnp.float32)
    hidden = (jax.nn.silu(gate_val) * up_val).astype(jnp.bfloat16)
    partial_value = jnp.einsum("emf,efd->emd", hidden, w_down, preferred_element_type=jnp.float32)
    partial_value = partial_value.reshape(local_experts, expert_count, item_rows, width_all)
    partial_value = partial_value.transpose(1, 0, 2, 3).reshape(experts_all, item_rows, width_all)
    summed = lax.psum_scatter(partial_value, "tensor", scatter_dimension=2, tiled=True).astype(
        jnp.bfloat16
    )
    returned = lax.all_to_all(summed, "expert", split_axis=0, concat_axis=0, tiled=True)
    shared_g = jnp.dot(tokens, shared_gate, preferred_element_type=jnp.float32)
    shared_u = jnp.dot(tokens, shared_up, preferred_element_type=jnp.float32)
    shared_hidden = (jax.nn.silu(shared_g) * shared_u).astype(jnp.bfloat16)
    shared_part = jnp.dot(shared_hidden, shared_down, preferred_element_type=jnp.float32)
    picked = returned.reshape(experts_all * capacity, half_width)[slot_index]
    picked = picked.astype(jnp.float32).reshape(tok_count, top_count, half_width)
    routed = jnp.sum(gates[:, :, None] * picked, axis=1)
    total = routed + lax.psum_scatter(shared_part, "tensor", scatter_dimension=1, tiled=True)
    return (own_cols.astype(jnp.float32) + total).astype(jnp.bfloat16)


def silu_mul(g, u):
    return (g / (1.0 + jnp.exp(-g)) * u).astype(jnp.bfloat16)


def moe_kernel(nz, nx, cap, tok_ref, routes_ref, gates_ref, wg_ref, wu_ref, wd_ref, sg_ref, su_ref, sd_ref, out_ref,
               TOK, X, XC, XO, XIN, YS, YC, CSs, CSr, MRG, BS, BR, AR, OWN, O, SHB, SHr, MT, POS, WT, U, Wg, Wu, Wd, Sg, Su, Sd,
               t_loc, w_loc, s_loc, w_send, w_recv, m_send, m_recv, q_send, q_recv, z_send, z_recv, x_send, x_recv, d_send, d_recv,
               y_send, y_recv, e_send, e_recv, f_send, f_recv,
               a_send, a_recv, b_send, b_recv, c_send, c_recv, g_recv, h_send, h_recv):
    bf, f32 = jnp.bfloat16, jnp.float32
    me = lax.axis_index("expert")
    core = lax.axis_index("tensor")
    z = me // nx
    x = me % nx
    ox = nx - 1 - x
    other = z * nx + ox
    n = nz * nx
    half, rows = out_ref.shape
    ch = cap // 2
    top = routes_ref.shape[0]
    chunks = z_recv.shape[1]
    part = half // chunks
    sum_chunks = c_send.shape[1]
    sum_part = half // sum_chunks

    barrier = pltpu.get_barrier_semaphore()
    for d in range(1, nz):
        peer = ((z + d) % nz) * nx + x
        pl.semaphore_signal(barrier, inc=1, device_id={"expert": peer}, device_id_type=MESH)
    pl.semaphore_signal(barrier, inc=1, device_id={"expert": other}, device_id_type=MESH)
    pl.semaphore_signal(barrier, inc=1, device_id={"tensor": 1 - core}, device_id_type=MESH)
    pl.semaphore_signal(barrier, inc=1, device_id={"expert": other, "tensor": 1 - core}, device_id_type=MESH)

    own_in = pltpu.make_async_copy(tok_ref.at[pl.ds(pl.multiple_of(core * half, 16), half)], X.at[z], t_loc.at[0])
    tok_in = pltpu.make_async_copy(tok_ref, TOK, t_loc.at[1])
    own_in.start()
    tok_in.start()
    loc_s = [pltpu.make_async_copy(a, b, s_loc.at[i]) for i, (a, b) in enumerate(
        ((sg_ref, Sg), (su_ref, Su), (sd_ref, Sd)))]
    loc_w = [pltpu.make_async_copy(a.at[0], b.at[0], w_loc.at[i]) for i, (a, b) in enumerate(
        ((wg_ref, Wg), (wu_ref, Wu), (wd_ref, Wd)))]
    for cp in loc_s + loc_w:
        cp.start()

    def remote(src, dst, ssem, rsem, **dev):
        return pltpu.make_async_remote_copy(src_ref=src, dst_ref=dst, send_sem=ssem, recv_sem=rsem,
                                            device_id=dev, device_id_type=MESH)

    MT[me, :top] = routes_ref[...].astype(f32)
    MT[me, top:] = gates_ref[...]
    U[...] = jnp.where(lax.broadcasted_iota(jnp.int32, U.shape, 0) < lax.broadcasted_iota(jnp.int32, U.shape, 1),
                       1.0, 0.0).astype(bf)

    def ranks(e):
        named, gate = MT[e, :top], MT[e, top:]
        mine, theirs = named == me.astype(f32), named == other.astype(f32)

        def over(value):
            return jnp.concatenate([jnp.sum(jnp.where(hit, value, 0.0), axis=0, keepdims=True)
                                    for hit in (mine, theirs)], axis=0)
        on, weight = over(1.0), over(gate)
        place = jnp.dot(on.astype(bf), U[...], preferred_element_type=f32)
        place = jnp.where(on > 0, place, -1.0)
        for k in range(2):
            POS[pl.ds(k * n + e, 1), :] = place[k:k + 1]
            WT[pl.ds(k * n + e, 1), :] = weight[k:k + 1]

    ranks(me)
    own_in.wait()
    pl.semaphore_wait(barrier, nz + 2)

    def m_copy(zo, side):
        e = zo * nx + x
        return remote(MT.at[e], MT.at[e], m_send.at[side, zo], m_recv.at[zo], expert=me + nx if side == 0 else me - nx)

    def q_copy(e):
        return remote(MT.at[e], MT.at[e], q_send, q_recv, expert=other)

    def f_copy(zo, source):
        r = pl.ds(pl.multiple_of(cap + source * ch, ch), ch)
        return remote(YS.at[zo, 1 - core, pl.ds(ch, ch)], YC.at[zo, r], f_send, f_recv, tensor=1 - core)

    def b_copy(k):
        r = pl.ds(k * sum_part, sum_part)
        return remote(BS.at[r], BR.at[r], b_send.at[k], b_recv.at[k], expert=jnp.where(z == 0, me + nx, me - nx))

    def a_copy(k):
        r = pl.ds(k * sum_part, sum_part)
        return remote(BS.at[r], AR.at[r], a_send.at[k], a_recv.at[k], expert=other)

    def z_copy(zo, side, k):
        r = pl.ds(k * part, part)
        return remote(X.at[zo, r], X.at[zo, r], z_send.at[side, zo, k], z_recv.at[zo, k],
                      expert=me + nx if side == 0 else me - nx)

    def x_copy(zo, k, source):
        return remote(XC.at[zo, pl.ds(k * ch, ch)], XIN.at[zo, source, pl.ds(ch, ch)], x_send.at[k, zo],
                      x_recv.at[source, zo], expert=other, tensor=k)

    def d_copy(zo, source):
        return remote(XO.at[zo], XIN.at[zo, source, pl.ds(0, ch)], d_send.at[zo], d_recv.at[zo], tensor=1 - core)

    def y_copy(zo, k, source):
        r = pl.ds(pl.multiple_of(cap + source * ch, ch), ch)
        return remote(YS.at[zo, k, pl.ds(ch, ch)], YC.at[zo, r], y_send.at[k, zo], y_recv.at[source, zo],
                      expert=other, tensor=k)

    def e_copy(zo, source):
        r = pl.ds(pl.multiple_of(source * ch, ch), ch)
        return remote(YS.at[zo, 1 - core, pl.ds(0, ch)], YC.at[zo, r], e_send.at[zo], e_recv.at[zo], tensor=1 - core)

    def c_copy(zo, slot, k):
        r = pl.ds(k * sum_part, sum_part)
        return remote(CSs.at[zo, r], CSr.at[slot, r], c_send.at[zo, k], c_recv.at[slot, k], expert=zo * nx + x)

    def g_copy(zo, k):
        r = pl.ds(k * sum_part, sum_part)
        return remote(CSs.at[zo, r], MRG.at[zo, r], c_send.at[zo, k], g_recv.at[zo, k],
                      expert=jnp.where(z == 0, me + nx, me - nx))

    def forward(zo, start):
        @pl.when(jnp.logical_and(zo <= z, z + 1 < nz))
        def _():
            start(0)

        @pl.when(jnp.logical_and(zo >= z, z >= 1))
        def _():
            start(1)

    def forward_m(zo):
        forward(zo, lambda side: m_copy(zo, side).start())

    def forward_z(zo, k):
        forward(zo, lambda side: z_copy(zo, side, k).start())

    def take_z(zo):
        m_copy(zo, 0).wait_recv()
        forward_m(zo)
        ranks(zo * nx + x)
        for k in range(chunks):
            z_copy(zo, 0, k).wait_recv()
            forward_z(zo, k)

    def spread(zo):
        e = zo * nx + x
        r = lax.broadcasted_iota(jnp.int32, (cap, rows), 0)
        near = jnp.where(r < ch, r + core * ch, r - ch + (1 - core) * ch).astype(f32)
        pick = jnp.concatenate([jnp.where(r.astype(f32) == POS[pl.ds(n + e, 1), :], 1.0, 0.0),
                                jnp.where(near == POS[pl.ds(e, 1), :], 1.0, 0.0)], axis=0).astype(bf)
        got = lax.dot_general(pick, X[zo], (((1,), (1,)), ((), ())), preferred_element_type=f32).astype(bf)
        XC[zo] = got[:cap]
        for k in range(2):
            x_copy(zo, k, core).start()
        XIN[zo, core, :ch] = got[cap:cap + ch]
        XO[zo] = got[cap + ch:]
        d_copy(zo, core).start()

    forward_m(z)
    for k in range(chunks):
        forward_z(z, k)
    spread(z)
    edge = jnp.logical_or(z == 0, z == nz - 1)

    @pl.when(jnp.logical_not(edge))
    def _():
        q_copy(me).start()
    rem_w = [remote(a.at[0], b.at[1], w_send.at[i], w_recv.at[i], tensor=1 - core) for i, (a, b) in enumerate(
        ((wg_ref, Wg), (wu_ref, Wu), (wd_ref, Wd)))]
    for cp in rem_w:
        cp.start()

    table = [sorted(range(nz), key=lambda q: (abs(q - k), abs(2 * q + 1 - nz))) for k in range(nz)]

    def nth(i):
        r = table[0][i]
        for k in range(1, nz):
            r = jnp.where(z == k, table[k][i], r)
        return r

    for cp in loc_s:
        cp.wait()
    tok_in.wait()
    tok = TOK[...].T
    sh = silu_mul(jnp.dot(tok, Sg[...], preferred_element_type=f32),
                  jnp.dot(tok, Su[...], preferred_element_type=f32))
    sh_all = jnp.dot(sh, Sd[...], preferred_element_type=f32).T
    SHB[0] = sh_all[:half]
    SHB[1] = sh_all[half:]
    h_copy = remote(SHB.at[1 - core], SHr, h_send, h_recv, tensor=1 - core)
    h_copy.start()

    for cp in loc_w:
        cp.wait()
    for cp in rem_w:
        cp.wait_recv()

    def compute(zo):
        d_copy(zo, 1 - core).wait_recv()
        for s in range(2):
            x_copy(zo, s, s).wait_recv()
        for hh in range(2):
            parts = []
            for w in (Wg, Wu):
                parts.append(jnp.dot(XIN[zo, 0], w[hh, :half], preferred_element_type=f32)
                             + jnp.dot(XIN[zo, 1], w[hh, half:], preferred_element_type=f32))
            down = jnp.dot(silu_mul(*parts), Wd[hh], preferred_element_type=f32)
            if hh == 0:
                O[...] = down
            else:
                O[...] += down
        y = O[...].astype(bf)
        YS[zo, 0] = y[:, :half]
        YS[zo, 1] = y[:, half:]

    def give_near(zo):
        e_copy(zo, core).start()
        YC[zo, pl.ds(pl.multiple_of(core * ch, ch), ch)] = YS[zo, core, :ch]

    def give_far(zo):
        for k in range(2):
            y_copy(zo, k, core).start()

    def keep_far(zo):
        f_copy(zo, core).start()
        YC[zo, pl.ds(pl.multiple_of(cap + core * ch, ch), ch)] = YS[zo, core, ch:]

    def put(rows_of):
        slot = lax.broadcasted_iota(jnp.int32, (cap, rows), 0).astype(f32)
        return jnp.concatenate([jnp.where(slot == POS[pl.ds(q, 1), :], WT[pl.ds(q, 1), :], 0.0)
                                for q in rows_of], axis=0).astype(bf)

    def back(values, rows_of):
        return lax.dot_general(values, put(rows_of), (((0,), (0,)), ((), ())), preferred_element_type=f32)

    def column(zo, whole):
        e = zo * nx + x
        e_copy(zo, 1 - core).wait_recv()
        if not whole:
            return back(YC[zo, :cap], (e,))
        for s in range(2):
            y_copy(zo, s, s).wait_recv()
        return back(YC[zo], (e, n + e))

    def others(zo):
        f_copy(zo, 1 - core).wait_recv()
        e = zo * nx + ox
        q_copy(e).wait_recv()
        ranks(e)
        return back(YC[zo, cap:], (e,))

    def give(i, on_edge):
        if i == 0 and not on_edge:
            dense = others(z)
            for k in range(sum_chunks):
                r = slice(k * sum_part, (k + 1) * sum_part)
                b_copy(k).wait_recv()
                BS[r] = (dense[r] + BR[r].astype(f32)).astype(bf)
                a_copy(k).start()
        else:
            give_far(nth(i))

    def column_sum(i, on_edge):
        zo = nth(i)
        if on_edge and i == 1:
            BS[...] = others(zo).astype(bf)
            for k in range(sum_chunks):
                b_copy(k).start()
        summed = column(zo, i != (1 if on_edge else 0))
        if i == 0:
            OWN[...] = X[z].astype(f32) + summed
            if not on_edge:
                for k in range(sum_chunks):
                    a_copy(k).wait_recv()
                OWN[...] += AR[...].astype(f32)
            return
        for k in range(sum_chunks):
            r = slice(k * sum_part, (k + 1) * sum_part)
            piece = summed[r]
            if not on_edge and i in MERGED:
                g_copy(zo, k).wait_recv()
                piece = piece + MRG[zo, r].astype(f32)
            CSs[zo, r] = piece.astype(bf)
            if on_edge and i in RELAYED:
                g_copy(zo, k).start()
            else:
                c_copy(zo, z, k).start()

    def run(steps, on_edge):
        for op, i in steps:
            if op == "take":
                take_z(nth(i))
            elif op == "spread":
                spread(nth(i))
                if on_edge and i == 1:
                    q_copy(nth(i) * nx + x).start()
            elif op == "give":
                give(i, on_edge)
            else:
                column_sum(i, on_edge)

    def cut(order):
        gaps, firsts = [[]], []
        for op, i in order:
            if op == "compute":
                firsts.append(i)
                gaps.append([])
            else:
                gaps[-1].append((op, i))
        return gaps, firsts

    edge_gaps, edge_first = cut(EDGE_ORDER)
    inner_gaps, inner_first = cut(INNER_ORDER)
    for j in range(nz + 1):
        @pl.when(edge)
        def _():
            run(edge_gaps[j], True)

        @pl.when(jnp.logical_not(edge))
        def _():
            run(inner_gaps[j], False)
        if j < nz:
            zi = jnp.where(edge, nth(edge_first[j]), nth(inner_first[j]))
            compute(zi)
            give_near(zi)
            if edge_first[j] == 1 and inner_first[j] == 0:
                keep_far(zi)
            elif edge_first[j] == 1:
                pl.when(edge)(lambda: keep_far(zi))
            elif inner_first[j] == 0:
                pl.when(jnp.logical_not(edge))(lambda: keep_far(zi))
    h_copy.wait_recv()
    OWN[...] += SHB[core] + SHr[...]
    for k in range(sum_chunks):
        r = slice(k * sum_part, (k + 1) * sum_part)
        total = OWN[r]
        for i in SOURCES:
            zi = nth(i)
            c_copy(zi, zi, k).wait_recv()
            total = total + CSr[zi, r].astype(f32)
        out_ref[r] = total.astype(bf)

    for cp in rem_w:
        cp.wait_send()
    h_copy.wait_send()
    q_copy(me).wait_send()
    f_copy(z, core).wait_send()

    @pl.when(edge)
    def _():
        for k in range(sum_chunks):
            b_copy(k).wait_send()

    @pl.when(jnp.logical_not(edge))
    def _():
        for k in range(sum_chunks):
            a_copy(k).wait_send()
    for i in range(nz):
        zo = nth(i)
        forward(zo, lambda side: m_copy(zo, side).wait_send())
        for k in range(chunks):
            forward(zo, lambda side: z_copy(zo, side, k).wait_send())
        for k in range(2):
            x_copy(zo, k, core).wait_send()
        d_copy(zo, core).wait_send()
        e_copy(zo, core).wait_send()

        def sent():
            for k in range(2):
                y_copy(zo, k, core).wait_send()
        if i == 0:
            pl.when(edge)(sent)
        elif i == 1:
            pl.when(jnp.logical_not(edge))(sent)
        else:
            sent()
        if i > 0:
            for k in range(sum_chunks):
                c_copy(zo, z, k).wait_send()


def pad(n, m):
    return -(-n // m) * m


def most_named(tok_count, top_count, experts_all):
    return max(2, (3 * tok_count * top_count + 2 * experts_all - 1) // (2 * experts_all))


def gather_plan(tok_count, width, expert_count, local_experts, hidden, top_count):
    cap = most_named(tok_count, top_count, expert_count)
    if local_experts != 1 or expert_count != 2 * LINE or tok_count % 256 or width % 32 or cap % 32 or cap > tok_count:
        return None
    nz, half = expert_count // 2, pad(width // 2, 128)
    wide, hid = pad(width, 128), pad(hidden, 128)
    weights = 3 * (2 * width * hid + pad(hidden, 16) * wide) * 2
    moved = nz * half * 2 * (4 * tok_count + 2 * cap + 2 * cap + 2 * cap + 2 * cap)
    flat = tok_count * (wide * 2 + 4 * half * 4 + 8 * half) + cap * wide * 4 + 4 * tok_count * tok_count
    return weights + moved + flat


def gather_local(tokens, routes, gates, w_gate, w_up, w_down, shared_gate, shared_up, shared_down):
    tok_count, width = tokens.shape
    hidden = w_gate.shape[2]
    n = lax.axis_size("expert")
    top = routes.shape[1]
    nx, nz = 2, n // 2
    half = width // 2
    cap = most_named(tok_count, top, n)
    ch = cap // 2
    chunks = next(c for c in (3, 2, 1) if half % (16 * c) == 0)
    sums = chunks
    bf, f32 = jnp.bfloat16, jnp.float32
    vm, dma = pltpu.VMEM, pltpu.SemaphoreType.DMA
    scratch = [
        vm((width, tok_count), bf), vm((nz, half, tok_count), bf), vm((nz, cap, half), bf), vm((nz, ch, half), bf),
        vm((nz, 2, cap, half), bf), vm((nz, 2, cap, half), bf), vm((nz, 2 * cap, half), bf),
        vm((nz, half, tok_count), bf), vm((nz, half, tok_count), bf), vm((nz, half, tok_count), bf),
        vm((half, tok_count), bf), vm((half, tok_count), bf), vm((half, tok_count), bf), vm((half, tok_count), f32),
        vm((cap, width), f32), vm((2, half, tok_count), f32), vm((half, tok_count), f32),
        vm((n, 2 * top, tok_count), f32), vm((2 * n, tok_count), f32), vm((2 * n, tok_count), f32),
        vm((tok_count, tok_count), bf),
        vm((2, width, hidden), bf), vm((2, width, hidden), bf), vm((2, hidden, width), bf),
        vm((width, hidden), bf), vm((width, hidden), bf), vm((hidden, width), bf),
        dma((2,)), dma((3,)), dma((3,)), dma((3,)), dma((3,)), dma((2, nz)), dma((nz,)), dma, dma,
        dma((2, nz, chunks)), dma((nz, chunks)), dma((2, nz)), dma((2, nz)), dma((nz,)), dma((nz,)),
        dma((2, nz)), dma((2, nz)), dma((nz,)), dma((nz,)), dma, dma, dma((sums,)), dma((sums,)), dma((sums,)), dma((sums,)),
        dma((nz, sums)), dma((nz, sums)), dma((nz, sums)), dma, dma,
    ]
    in_vmem, in_hbm = pl.BlockSpec(memory_space=pltpu.VMEM), pl.BlockSpec(memory_space=pl.ANY)
    return pl.pallas_call(
        functools.partial(moe_kernel, nz, nx, cap),
        out_shape=jax.ShapeDtypeStruct((half, tok_count), bf),
        in_specs=[in_hbm] + [in_vmem] * 2 + [in_hbm] * 6,
        out_specs=in_vmem,
        scratch_shapes=scratch,
        compiler_params=pltpu.CompilerParams(collective_id=0, has_side_effects=True, vmem_limit_bytes=60 * 1024 * 1024),
    )(tokens.T, routes.T, gates.T, w_gate, w_up, w_down, shared_gate, shared_up, shared_down).T


def local(tokens, routes, gates, w_gate, *rest):
    need = gather_plan(*tokens.shape, lax.axis_size("expert"), w_gate.shape[0], w_gate.shape[2], routes.shape[1])
    if need is not None and lax.axis_size("tensor") == 2 and need <= VMEM_BUDGET:
        return gather_local(tokens, routes, gates, w_gate, *rest)
    return exchange_local(tokens, routes, gates, w_gate, *rest)


def solution(mesh):
    in_specs = (
        P(("groups", "expert"), None),
        P(("groups", "expert"), None),
        P(("groups", "expert"), None),
        P("expert", None, "tensor"),
        P("expert", None, "tensor"),
        P("expert", "tensor", None),
        P(None, "tensor"),
        P(None, "tensor"),
        P("tensor", None),
    )
    out_specs = P(("groups", "expert"), "tensor")
    return jax.shard_map(local, mesh=mesh, in_specs=in_specs, out_specs=out_specs, check_vma=False)
```

```python
import functools

import jax
import jax.numpy as jnp
from jax import lax
from jax.experimental import pallas as pl
from jax.experimental.pallas import tpu as pltpu
from jax.sharding import PartitionSpec as P

MESH = pl.DeviceIdType.MESH
VMEM_BUDGET = 52 * 1024 * 1024
LINE = 4
EDGE_ORDER = (
    ("take", 1), ("spread", 1), ("compute", 0), ("take", 2), ("spread", 2), ("compute", 1), ("sum", 1),
    ("take", 3), ("spread", 3), ("compute", 2), ("give", 2), ("compute", 3), ("give", 3), ("sum", 2), ("give",
    0), ("sum", 3), ("sum", 0),
)
INNER_ORDER = (
    ("take", 1), ("spread", 1), ("take", 2), ("spread", 2), ("take", 3), ("spread", 3), ("compute", 1),
    ("compute", 2), ("give", 2), ("compute", 0), ("give", 1), ("compute", 3), ("give", 3), ("sum", 2),
    ("give", 0), ("sum", 1), ("sum", 3), ("sum", 0),
)
RELAYED, MERGED, SOURCES = (2, 3), (1, 3), (1, 2)


def exchange_local(tokens, routes, gates, w_gate, w_up, w_down, shared_gate, shared_up, shared_down):
    tok_count, top_count = routes.shape
    width_all = tokens.shape[1]
    local_experts = w_gate.shape[0]
    expert_count = lax.axis_size("expert")
    experts_all = expert_count * local_experts
    capacity = max(2, (3 * tok_count * top_count + 2 * experts_all - 1) // (2 * experts_all))
    flat_routes = routes.reshape(-1)
    onehot = (flat_routes[:, None] == jnp.arange(experts_all, dtype=jnp.int32)[None, :]).astype(
        jnp.int32
    )
    order_in = jnp.sum(jnp.cumsum(onehot, axis=0) * onehot, axis=1) - 1
    slot_index = flat_routes * capacity + order_in
    half_width = width_all // lax.axis_size("tensor")
    own_cols = lax.dynamic_slice_in_dim(
        tokens, lax.axis_index("tensor") * half_width, half_width, 1
    )
    outgoing = jnp.zeros((experts_all * capacity, half_width), jnp.bfloat16)
    outgoing = outgoing.at[slot_index].set(jnp.repeat(own_cols, top_count, axis=0))
    outgoing = outgoing.reshape(experts_all, capacity, half_width)
    received = lax.all_to_all(outgoing, "expert", split_axis=0, concat_axis=0, tiled=True)
    received = lax.all_gather(received, "tensor", axis=2, tiled=True)
    item_rows = received.shape[1]
    stacked = received.reshape(expert_count, local_experts, item_rows, width_all)
    stacked = stacked.transpose(1, 0, 2, 3).reshape(
        local_experts, expert_count * item_rows, width_all
    )
    gate_val = jnp.einsum("emd,edf->emf", stacked, w_gate, preferred_element_type=jnp.float32)
    up_val = jnp.einsum("emd,edf->emf", stacked, w_up, preferred_element_type=jnp.float32)
    hidden = (jax.nn.silu(gate_val) * up_val).astype(jnp.bfloat16)
    partial_value = jnp.einsum("emf,efd->emd", hidden, w_down, preferred_element_type=jnp.float32)
    partial_value = partial_value.reshape(local_experts, expert_count, item_rows, width_all)
    partial_value = partial_value.transpose(1, 0, 2, 3).reshape(experts_all, item_rows, width_all)
    summed = lax.psum_scatter(partial_value, "tensor", scatter_dimension=2, tiled=True).astype(
        jnp.bfloat16
    )
    returned = lax.all_to_all(summed, "expert", split_axis=0, concat_axis=0, tiled=True)
    shared_g = jnp.dot(tokens, shared_gate, preferred_element_type=jnp.float32)
    shared_u = jnp.dot(tokens, shared_up, preferred_element_type=jnp.float32)
    shared_hidden = (jax.nn.silu(shared_g) * shared_u).astype(jnp.bfloat16)
    shared_part = jnp.dot(shared_hidden, shared_down, preferred_element_type=jnp.float32)
    picked = returned.reshape(experts_all * capacity, half_width)[slot_index]
    picked = picked.astype(jnp.float32).reshape(tok_count, top_count, half_width)
    routed = jnp.sum(gates[:, :, None] * picked, axis=1)
    total = routed + lax.psum_scatter(shared_part, "tensor", scatter_dimension=1, tiled=True)
    return (own_cols.astype(jnp.float32) + total).astype(jnp.bfloat16)


def silu_mul(g, u):
    return (g / (1.0 + jnp.exp(-g)) * u).astype(jnp.bfloat16)


def moe_kernel(nz, nx, cap, tok_ref, routes_ref, gates_ref, wg_ref, wu_ref, wd_ref, sg_ref, su_ref, sd_ref, out_ref,
               TOK, X, XC, XO, XIN, YS, YC, CSs, CSr, MRG, BS, BR, AR, OWN, O, SHB, SHr, MT, POS, WT, U, Wg, Wu, Wd, Sg, Su, Sd,
               t_loc, w_loc, s_loc, w_send, w_recv, m_send, m_recv, q_send, q_recv, z_send, z_recv, x_send, x_recv, d_send, d_recv,
               y_send, y_recv, e_send, e_recv, f_send, f_recv,
               a_send, a_recv, b_send, b_recv, c_send, c_recv, g_recv, h_send, h_recv):
    bf, f32 = jnp.bfloat16, jnp.float32
    me = lax.axis_index("expert")
    core = lax.axis_index("tensor")
    z = me // nx
    x = me % nx
    ox = nx - 1 - x
    other = z * nx + ox
    n = nz * nx
    half, rows = out_ref.shape
    ch = cap // 2
    top = routes_ref.shape[0]
    chunks = z_recv.shape[1]
    part = half // chunks
    sum_chunks = c_send.shape[1]
    sum_part = half // sum_chunks

    barrier = pltpu.get_barrier_semaphore()
    for d in range(1, nz):
        peer = ((z + d) % nz) * nx + x
        pl.semaphore_signal(barrier, inc=1, device_id={"expert": peer}, device_id_type=MESH)
    pl.semaphore_signal(barrier, inc=1, device_id={"expert": other}, device_id_type=MESH)
    pl.semaphore_signal(barrier, inc=1, device_id={"tensor": 1 - core}, device_id_type=MESH)
    pl.semaphore_signal(barrier, inc=1, device_id={"expert": other, "tensor": 1 - core}, device_id_type=MESH)

    own_in = pltpu.make_async_copy(tok_ref.at[pl.ds(pl.multiple_of(core * half, 16), half)], X.at[z], t_loc.at[0])
    tok_in = pltpu.make_async_copy(tok_ref, TOK, t_loc.at[1])
    own_in.start()
    tok_in.start()
    loc_s = [pltpu.make_async_copy(a, b, s_loc.at[i]) for i, (a, b) in enumerate(
        ((sg_ref, Sg), (su_ref, Su), (sd_ref, Sd)))]
    loc_w = [pltpu.make_async_copy(a.at[0], b.at[0], w_loc.at[i]) for i, (a, b) in enumerate(
        ((wg_ref, Wg), (wu_ref, Wu), (wd_ref, Wd)))]
    for cp in loc_s + loc_w:
        cp.start()

    def remote(src, dst, ssem, rsem, **dev):
        return pltpu.make_async_remote_copy(src_ref=src, dst_ref=dst, send_sem=ssem, recv_sem=rsem,
                                            device_id=dev, device_id_type=MESH)

    MT[me, :top] = routes_ref[...].astype(f32)
    MT[me, top:] = gates_ref[...]
    U[...] = jnp.where(lax.broadcasted_iota(jnp.int32, U.shape, 0) < lax.broadcasted_iota(jnp.int32, U.shape, 1),
                       1.0, 0.0).astype(bf)

    def ranks(e):
        named, gate = MT[e, :top], MT[e, top:]
        mine, theirs = named == me.astype(f32), named == other.astype(f32)

        def over(value):
            return jnp.concatenate([jnp.sum(jnp.where(hit, value, 0.0), axis=0, keepdims=True)
                                    for hit in (mine, theirs)], axis=0)
        on, weight = over(1.0), over(gate)
        place = jnp.dot(on.astype(bf), U[...], preferred_element_type=f32)
        place = jnp.where(on > 0, place, -1.0)
        for k in range(2):
            POS[pl.ds(k * n + e, 1), :] = place[k:k + 1]
            WT[pl.ds(k * n + e, 1), :] = weight[k:k + 1]

    ranks(me)
    own_in.wait()
    pl.semaphore_wait(barrier, nz + 2)

    def m_copy(zo, side):
        e = zo * nx + x
        return remote(MT.at[e], MT.at[e], m_send.at[side, zo], m_recv.at[zo], expert=me + nx if side == 0 else me - nx)

    def q_copy(e):
        return remote(MT.at[e], MT.at[e], q_send, q_recv, expert=other)

    def f_copy(zo, source):
        r = pl.ds(pl.multiple_of(cap + source * ch, ch), ch)
        return remote(YS.at[zo, 1 - core, pl.ds(ch, ch)], YC.at[zo, r], f_send, f_recv, tensor=1 - core)

    def b_copy(k):
        r = pl.ds(k * sum_part, sum_part)
        return remote(BS.at[r], BR.at[r], b_send.at[k], b_recv.at[k], expert=jnp.where(z == 0, me + nx, me - nx))

    def a_copy(k):
        r = pl.ds(k * sum_part, sum_part)
        return remote(BS.at[r], AR.at[r], a_send.at[k], a_recv.at[k], expert=other)

    def z_copy(zo, side, k):
        r = pl.ds(k * part, part)
        return remote(X.at[zo, r], X.at[zo, r], z_send.at[side, zo, k], z_recv.at[zo, k],
                      expert=me + nx if side == 0 else me - nx)

    def x_copy(zo, k, source):
        return remote(XC.at[zo, pl.ds(k * ch, ch)], XIN.at[zo, source, pl.ds(ch, ch)], x_send.at[k, zo],
                      x_recv.at[source, zo], expert=other, tensor=k)

    def d_copy(zo, source):
        return remote(XO.at[zo], XIN.at[zo, source, pl.ds(0, ch)], d_send.at[zo], d_recv.at[zo], tensor=1 - core)

    def y_copy(zo, k, source):
        r = pl.ds(pl.multiple_of(cap + source * ch, ch), ch)
        return remote(YS.at[zo, k, pl.ds(ch, ch)], YC.at[zo, r], y_send.at[k, zo], y_recv.at[source, zo],
                      expert=other, tensor=k)

    def e_copy(zo, source):
        r = pl.ds(pl.multiple_of(source * ch, ch), ch)
        return remote(YS.at[zo, 1 - core, pl.ds(0, ch)], YC.at[zo, r], e_send.at[zo], e_recv.at[zo], tensor=1 - core)

    def c_copy(zo, slot, k):
        r = pl.ds(k * sum_part, sum_part)
        return remote(CSs.at[zo, r], CSr.at[slot, r], c_send.at[zo, k], c_recv.at[slot, k], expert=zo * nx + x)

    def g_copy(zo, k):
        r = pl.ds(k * sum_part, sum_part)
        return remote(CSs.at[zo, r], MRG.at[zo, r], c_send.at[zo, k], g_recv.at[zo, k],
                      expert=jnp.where(z == 0, me + nx, me - nx))

    def forward(zo, start):
        @pl.when(jnp.logical_and(zo <= z, z + 1 < nz))
        def _():
            start(0)

        @pl.when(jnp.logical_and(zo >= z, z >= 1))
        def _():
            start(1)

    def forward_m(zo):
        forward(zo, lambda side: m_copy(zo, side).start())

    def forward_z(zo, k):
        forward(zo, lambda side: z_copy(zo, side, k).start())

    def take_z(zo):
        m_copy(zo, 0).wait_recv()
        forward_m(zo)
        ranks(zo * nx + x)
        for k in range(chunks):
            z_copy(zo, 0, k).wait_recv()
            forward_z(zo, k)

    def spread(zo):
        e = zo * nx + x
        r = lax.broadcasted_iota(jnp.int32, (cap, rows), 0)
        near = jnp.where(r < ch, r + core * ch, r - ch + (1 - core) * ch).astype(f32)
        pick = jnp.concatenate([jnp.where(r.astype(f32) == POS[pl.ds(n + e, 1), :], 1.0, 0.0),
                                jnp.where(near == POS[pl.ds(e, 1), :], 1.0, 0.0)], axis=0).astype(bf)
        got = lax.dot_general(pick, X[zo], (((1,), (1,)), ((), ())), preferred_element_type=f32).astype(bf)
        XC[zo] = got[:cap]
        for k in range(2):
            x_copy(zo, k, core).start()
        XIN[zo, core, :ch] = got[cap:cap + ch]
        XO[zo] = got[cap + ch:]
        d_copy(zo, core).start()

    forward_m(z)
    for k in range(chunks):
        forward_z(z, k)
    spread(z)
    edge = jnp.logical_or(z == 0, z == nz - 1)

    @pl.when(jnp.logical_not(edge))
    def _():
        q_copy(me).start()
    rem_w = [remote(a.at[0], b.at[1], w_send.at[i], w_recv.at[i], tensor=1 - core) for i, (a, b) in enumerate(
        ((wg_ref, Wg), (wu_ref, Wu), (wd_ref, Wd)))]
    for cp in rem_w:
        cp.start()

    table = [sorted(range(nz), key=lambda q: (abs(q - k), abs(2 * q + 1 - nz))) for k in range(nz)]

    def nth(i):
        r = table[0][i]
        for k in range(1, nz):
            r = jnp.where(z == k, table[k][i], r)
        return r

    for cp in loc_s:
        cp.wait()
    tok_in.wait()
    tok = TOK[...].T
    sh = silu_mul(jnp.dot(tok, Sg[...], preferred_element_type=f32),
                  jnp.dot(tok, Su[...], preferred_element_type=f32))
    sh_all = jnp.dot(sh, Sd[...], preferred_element_type=f32).T
    SHB[0] = sh_all[:half]
    SHB[1] = sh_all[half:]
    h_copy = remote(SHB.at[1 - core], SHr, h_send, h_recv, tensor=1 - core)
    h_copy.start()

    for cp in loc_w:
        cp.wait()
    for cp in rem_w:
        cp.wait_recv()

    def compute(zo):
        d_copy(zo, 1 - core).wait_recv()
        for s in range(2):
            x_copy(zo, s, s).wait_recv()
        for hh in range(2):
            parts = []
            for w in (Wg, Wu):
                parts.append(jnp.dot(XIN[zo, 0], w[hh, :half], preferred_element_type=f32)
                             + jnp.dot(XIN[zo, 1], w[hh, half:], preferred_element_type=f32))
            down = jnp.dot(silu_mul(*parts), Wd[hh], preferred_element_type=f32)
            if hh == 0:
                O[...] = down
            else:
                O[...] += down
        y = O[...].astype(bf)
        YS[zo, 0] = y[:, :half]
        YS[zo, 1] = y[:, half:]

    def give_near(zo):
        e_copy(zo, core).start()
        YC[zo, pl.ds(pl.multiple_of(core * ch, ch), ch)] = YS[zo, core, :ch]

    def give_far(zo):
        for k in range(2):
            y_copy(zo, k, core).start()

    def keep_far(zo):
        f_copy(zo, core).start()
        YC[zo, pl.ds(pl.multiple_of(cap + core * ch, ch), ch)] = YS[zo, core, ch:]

    def put(rows_of):
        slot = lax.broadcasted_iota(jnp.int32, (cap, rows), 0).astype(f32)
        return jnp.concatenate([jnp.where(slot == POS[pl.ds(q, 1), :], WT[pl.ds(q, 1), :], 0.0)
                                for q in rows_of], axis=0).astype(bf)

    def back(values, rows_of):
        return lax.dot_general(values, put(rows_of), (((0,), (0,)), ((), ())), preferred_element_type=f32)

    def column(zo, whole):
        e = zo * nx + x
        e_copy(zo, 1 - core).wait_recv()
        if not whole:
            return back(YC[zo, :cap], (e,))
        for s in range(2):
            y_copy(zo, s, s).wait_recv()
        return back(YC[zo], (e, n + e))

    def others(zo):
        f_copy(zo, 1 - core).wait_recv()
        e = zo * nx + ox
        q_copy(e).wait_recv()
        ranks(e)
        return back(YC[zo, cap:], (e,))

    def give(i, on_edge):
        if i == 0 and not on_edge:
            dense = others(z)
            for k in range(sum_chunks):
                r = slice(k * sum_part, (k + 1) * sum_part)
                b_copy(k).wait_recv()
                BS[r] = (dense[r] + BR[r].astype(f32)).astype(bf)
                a_copy(k).start()
        else:
            give_far(nth(i))

    def column_sum(i, on_edge):
        zo = nth(i)
        if on_edge and i == 1:
            BS[...] = others(zo).astype(bf)
            for k in range(sum_chunks):
                b_copy(k).start()
        summed = column(zo, i != (1 if on_edge else 0))
        if i == 0:
            OWN[...] = X[z].astype(f32) + summed
            if not on_edge:
                for k in range(sum_chunks):
                    a_copy(k).wait_recv()
                OWN[...] += AR[...].astype(f32)
            return
        for k in range(sum_chunks):
            r = slice(k * sum_part, (k + 1) * sum_part)
            piece = summed[r]
            if not on_edge and i in MERGED:
                g_copy(zo, k).wait_recv()
                piece = piece + MRG[zo, r].astype(f32)
            CSs[zo, r] = piece.astype(bf)
            if on_edge and i in RELAYED:
                g_copy(zo, k).start()
            else:
                c_copy(zo, z, k).start()

    def run(steps, on_edge):
        for op, i in steps:
            if op == "take":
                take_z(nth(i))
            elif op == "spread":
                spread(nth(i))
                if on_edge and i == 1:
                    q_copy(nth(i) * nx + x).start()
            elif op == "give":
                give(i, on_edge)
            else:
                column_sum(i, on_edge)

    def cut(order):
        gaps, firsts = [[]], []
        for op, i in order:
            if op == "compute":
                firsts.append(i)
                gaps.append([])
            else:
                gaps[-1].append((op, i))
        return gaps, firsts

    edge_gaps, edge_first = cut(EDGE_ORDER)
    inner_gaps, inner_first = cut(INNER_ORDER)
    for j in range(nz + 1):
        @pl.when(edge)
        def _():
            run(edge_gaps[j], True)

        @pl.when(jnp.logical_not(edge))
        def _():
            run(inner_gaps[j], False)
        if j < nz:
            zi = jnp.where(edge, nth(edge_first[j]), nth(inner_first[j]))
            compute(zi)
            give_near(zi)
            if edge_first[j] == 1 and inner_first[j] == 0:
                keep_far(zi)
            elif edge_first[j] == 1:
                pl.when(edge)(lambda: keep_far(zi))
            elif inner_first[j] == 0:
                pl.when(jnp.logical_not(edge))(lambda: keep_far(zi))
    h_copy.wait_recv()
    OWN[...] += SHB[core] + SHr[...]
    for k in range(sum_chunks):
        r = slice(k * sum_part, (k + 1) * sum_part)
        total = OWN[r]
        for i in SOURCES:
            zi = nth(i)
            c_copy(zi, zi, k).wait_recv()
            total = total + CSr[zi, r].astype(f32)
        out_ref[r] = total.astype(bf)

    for cp in rem_w:
        cp.wait_send()
    h_copy.wait_send()
    q_copy(me).wait_send()
    f_copy(z, core).wait_send()

    @pl.when(edge)
    def _():
        for k in range(sum_chunks):
            b_copy(k).wait_send()

    @pl.when(jnp.logical_not(edge))
    def _():
        for k in range(sum_chunks):
            a_copy(k).wait_send()
    for i in range(nz):
        zo = nth(i)
        forward(zo, lambda side: m_copy(zo, side).wait_send())
        for k in range(chunks):
            forward(zo, lambda side: z_copy(zo, side, k).wait_send())
        for k in range(2):
            x_copy(zo, k, core).wait_send()
        d_copy(zo, core).wait_send()
        e_copy(zo, core).wait_send()

        def sent():
            for k in range(2):
                y_copy(zo, k, core).wait_send()
        if i == 0:
            pl.when(edge)(sent)
        elif i == 1:
            pl.when(jnp.logical_not(edge))(sent)
        else:
            sent()
        if i > 0:
            for k in range(sum_chunks):
                c_copy(zo, z, k).wait_send()


def pad(n, m):
    return -(-n // m) * m


def most_named(tok_count, top_count, experts_all):
    return max(2, (3 * tok_count * top_count + 2 * experts_all - 1) // (2 * experts_all))


def gather_plan(tok_count, width, expert_count, local_experts, hidden, top_count):
    cap = most_named(tok_count, top_count, expert_count)
    if local_experts != 1 or expert_count != 2 * LINE or tok_count % 256 or width % 32 or cap % 32 or cap > tok_count:
        return None
    nz, half = expert_count // 2, pad(width // 2, 128)
    wide, hid = pad(width, 128), pad(hidden, 128)
    weights = 3 * (2 * width * hid + pad(hidden, 16) * wide) * 2
    moved = nz * half * 2 * (4 * tok_count + 2 * cap + 2 * cap + 2 * cap + 2 * cap)
    flat = tok_count * (wide * 2 + 4 * half * 4 + 8 * half) + cap * wide * 4 + 4 * tok_count * tok_count
    return weights + moved + flat


def gather_local(tokens, routes, gates, w_gate, w_up, w_down, shared_gate, shared_up, shared_down):
    tok_count, width = tokens.shape
    hidden = w_gate.shape[2]
    n = lax.axis_size("expert")
    top = routes.shape[1]
    nx, nz = 2, n // 2
    half = width // 2
    cap = most_named(tok_count, top, n)
    ch = cap // 2
    chunks = next(c for c in (3, 2, 1) if half % (16 * c) == 0)
    sums = next(c for c in (5, 3, 2, 1) if half % (16 * c) == 0)
    bf, f32 = jnp.bfloat16, jnp.float32
    vm, dma = pltpu.VMEM, pltpu.SemaphoreType.DMA
    scratch = [
        vm((width, tok_count), bf), vm((nz, half, tok_count), bf), vm((nz, cap, half), bf), vm((nz, ch, half), bf),
        vm((nz, 2, cap, half), bf), vm((nz, 2, cap, half), bf), vm((nz, 2 * cap, half), bf),
        vm((nz, half, tok_count), bf), vm((nz, half, tok_count), bf), vm((nz, half, tok_count), bf),
        vm((half, tok_count), bf), vm((half, tok_count), bf), vm((half, tok_count), bf), vm((half, tok_count), f32),
        vm((cap, width), f32), vm((2, half, tok_count), f32), vm((half, tok_count), f32),
        vm((n, 2 * top, tok_count), f32), vm((2 * n, tok_count), f32), vm((2 * n, tok_count), f32),
        vm((tok_count, tok_count), bf),
        vm((2, width, hidden), bf), vm((2, width, hidden), bf), vm((2, hidden, width), bf),
        vm((width, hidden), bf), vm((width, hidden), bf), vm((hidden, width), bf),
        dma((2,)), dma((3,)), dma((3,)), dma((3,)), dma((3,)), dma((2, nz)), dma((nz,)), dma, dma,
        dma((2, nz, chunks)), dma((nz, chunks)), dma((2, nz)), dma((2, nz)), dma((nz,)), dma((nz,)),
        dma((2, nz)), dma((2, nz)), dma((nz,)), dma((nz,)), dma, dma, dma((sums,)), dma((sums,)), dma((sums,)), dma((sums,)),
        dma((nz, sums)), dma((nz, sums)), dma((nz, sums)), dma, dma,
    ]
    in_vmem, in_hbm = pl.BlockSpec(memory_space=pltpu.VMEM), pl.BlockSpec(memory_space=pl.ANY)
    return pl.pallas_call(
        functools.partial(moe_kernel, nz, nx, cap),
        out_shape=jax.ShapeDtypeStruct((half, tok_count), bf),
        in_specs=[in_hbm] + [in_vmem] * 2 + [in_hbm] * 6,
        out_specs=in_vmem,
        scratch_shapes=scratch,
        compiler_params=pltpu.CompilerParams(collective_id=0, has_side_effects=True, vmem_limit_bytes=60 * 1024 * 1024),
    )(tokens.T, routes.T, gates.T, w_gate, w_up, w_down, shared_gate, shared_up, shared_down).T


def local(tokens, routes, gates, w_gate, *rest):
    need = gather_plan(*tokens.shape, lax.axis_size("expert"), w_gate.shape[0], w_gate.shape[2], routes.shape[1])
    if need is not None and lax.axis_size("tensor") == 2 and need <= VMEM_BUDGET:
        return gather_local(tokens, routes, gates, w_gate, *rest)
    return exchange_local(tokens, routes, gates, w_gate, *rest)


def solution(mesh):
    in_specs = (
        P(("groups", "expert"), None),
        P(("groups", "expert"), None),
        P(("groups", "expert"), None),
        P("expert", None, "tensor"),
        P("expert", None, "tensor"),
        P("expert", "tensor", None),
        P(None, "tensor"),
        P(None, "tensor"),
        P("tensor", None),
    )
    out_specs = P(("groups", "expert"), "tensor")
    return jax.shard_map(local, mesh=mesh, in_specs=in_specs, out_specs=out_specs, check_vma=False)
```
